32 devices in a mesh: gx: 4 (over z), gy: 2 (over y), gz: 4 (over x, core).
Axes of the slice: x: 2, y: 2, z: 4, core: 2. Of those that a mesh axis runs over, the one named last changes fastest.
Arguments:
- coords: float32 [3, 65536], P(None, ('gx', 'gy', 'gz')), may hold values from 0 to 3
- anchor: float32 [3, 65536], P(None, ('gx', 'gy', 'gz')), may hold values from -73 to 76
- atom_types: int32 [65536], P(('gx', 'gy', 'gz')), may hold values from 0 to 63
- halo_send: int32 [27904], P(('gx', 'gy', 'gz')), may hold values from 0 to 2047, as said below
- neighbours: int32 [8192, 8], P(('gx', 'gy', 'gz')), may hold values from 0 to 364, as said below
- live_counts: int32 [8192], P(('gx', 'gy', 'gz')), may hold values from 1 to 8
- rep_coef: float32 [64], replicated, may hold values from 0.5 to 2
- disp_coef: float32 [64], replicated, may hold values from 0.2 to 1
- charge: float32 [64], replicated, may hold values from -1 to 1
- step_history: float32 [8, 3, 65536], P(None, None, ('gx', 'gy', 'gz')), may hold values from -9 to 9
- grad_history: float32 [8, 3, 65536], P(None, None, ('gx', 'gy', 'gz')), may hold values from -72 to 72, as said below
Outputs:
- new_coords: float32 [3, 65536], P(None, ('gx', 'gy', 'gz'))
- energy: float32 [], replicated
The draws below stay inside these ranges and needn't reach their ends.
Inputs may be any that keep to these rules, and one draw needn't show every extreme that they name: `halo_send`: each of a domain's seven blocks holds distinct local atom indices, rising. `neighbours`: slot 0 of row r is r mod 256, the row's own cluster. `grad_history`: the product of each entry with the matching step_history entry is not negative, and each pair's inner product is positive.
All inputs are finite; a program needn't handle non-finite values.
Results may differ from the reference program's by a relative error of at most 0.0003.
Values sent between devices are 32-bit elements; how exact they have to be, the bound alone decides.
No kernel may reach another device: no remote copies, remote signals or barrier semaphores. Data moves between devices by JAX's collectives and lax.ppermute only.
A program may use at most 64 MiB of HBM per device.

```python
import math
import jax
import jax.numpy as jnp
from jax import lax

ATOMS_DEV = 2048
MEMORY = 8
NB = 8
NTYPES = 64
CLUSTERS = 256
EXT_CLUSTERS = 365
DOMAINS = 32
ATOMS = 65536
N_GX = 4
N_GY = 2
N_GZ = 4


def export_sizes_drawn(atoms_local):
    face_rows = atoms_local // 8
    edge_rows = max(atoms_local // 64, 8)
    corner_rows = max(atoms_local // 512, 8)
    return [face_rows, face_rows, edge_rows, face_rows, edge_rows, edge_rows, corner_rows]


def draw_halo_send(key, part):
    size_list = export_sizes_drawn(ATOMS_DEV)

    def one_domain(sub_key):
        block_keys = jax.random.split(sub_key, 7)
        blocks = [jnp.sort(jax.random.permutation(block_keys[block_pos], ATOMS_DEV)[:size_list[block_pos]]) for block_pos in range(7)]
        return jnp.concatenate(blocks).astype(jnp.int32)
    domain_keys = jax.random.split(jax.random.fold_in(key, 3), DOMAINS)
    return jax.vmap(one_domain)(domain_keys).reshape(-1)


def draw_neighbours(key, part):
    picks = jax.random.randint(jax.random.fold_in(key, 5), (DOMAINS * CLUSTERS, NB), 0, EXT_CLUSTERS, dtype=jnp.int32)
    own_ids = jnp.arange(DOMAINS * CLUSTERS, dtype=jnp.int32) % CLUSTERS
    return picks.at[:, 0].set(own_ids)


def rough_field(sub_key, field_shape):
    return jnp.clip(jax.random.normal(sub_key, field_shape, jnp.float32), -4.0, 4.0)


def system_draw(key):
    coord_key, base_key, scale_key, ratio_key, curve_key, older_key = jax.random.split(jax.random.fold_in(key, 7), 6)
    hist_shape = (MEMORY, 3, ATOMS)
    base_draw = rough_field(base_key, hist_shape)
    older_draw = rough_field(older_key, (3, ATOMS))
    domain_ids = jnp.arange(ATOMS) // ATOMS_DEV
    rising = jnp.exp(jnp.log(3.0) * domain_ids / max(DOMAINS - 1, 1))
    jitter = jnp.exp(jax.random.uniform(scale_key, (DOMAINS,), jnp.float32, -0.3, 0.3))[domain_ids]
    step_draw = 0.5 * base_draw * rising * jitter
    older_steps = 0.5 * older_draw * rising * jitter
    ratio_draw = jnp.exp(jax.random.uniform(ratio_key, hist_shape, jnp.float32, jnp.log(0.25), jnp.log(4.0)))
    curvature = jnp.exp(jax.random.uniform(curve_key, (MEMORY, 1, 1), jnp.float32, jnp.log(0.5), jnp.log(2.0)))
    diff_draw = curvature * ratio_draw * step_draw
    coord_draw = jax.random.uniform(coord_key, (3, ATOMS), jnp.float32, 0.0, 3.0)
    anchor_draw = coord_draw - jnp.sum(step_draw, axis=0) - older_steps
    return (coord_draw, anchor_draw, step_draw, diff_draw)


def draw_coords(key, part):
    return system_draw(key)[0]


def draw_anchor(key, part):
    return system_draw(key)[1]


def draw_step_history(key, part):
    return system_draw(key)[2]


def draw_grad_history(key, part):
    return system_draw(key)[3]


def set_ends(result, rng, smallest, top_value):
    dims = result.shape
    spot = [jax.random.randint(jax.random.fold_in(rng, axis), (), 0, dims[axis]) for axis in range(len(dims))]
    result = result.at[tuple(spot)].set(smallest)
    longest = dims.index(max(dims))
    spot[longest] = (spot[longest] + 1) % dims[longest]
    return result.at[tuple(spot)].set(top_value)


def setup_inputs(seed: int = 0) -> dict:
    seeds = jax.random.split(jax.random.key(seed), 12)
    coords = draw_coords(jax.random.fold_in(seeds[11], 71), 0)
    anchor = draw_anchor(jax.random.fold_in(seeds[11], 71), 0)
    atom_types = set_ends(jax.random.randint(seeds[2], (ATOMS,), 0, NTYPES), jax.random.fold_in(seeds[2], 1), 0, NTYPES - 1).astype(jnp.int32)
    halo_send = draw_halo_send(jax.random.fold_in(seeds[11], 71), 0)
    neighbours = draw_neighbours(jax.random.fold_in(seeds[11], 71), 0)
    live_counts = set_ends(jax.random.randint(seeds[5], (DOMAINS * CLUSTERS,), 1, NB + 1), jax.random.fold_in(seeds[5], 1), 1, NB).astype(jnp.int32)
    rep_coef = jnp.clip(jnp.exp(jax.random.uniform(seeds[6], (NTYPES,), jnp.float32, math.log(0.5), math.log(2.0))), 0.5, 2.0)
    disp_coef = jnp.clip(jnp.exp(jax.random.uniform(seeds[7], (NTYPES,), jnp.float32, math.log(0.2), math.log(1.0))), 0.2, 1.0)
    charge = jnp.clip(jax.random.uniform(seeds[8], (NTYPES,), jnp.float32, -1.0, 1.0), -1.0, 1.0)
    step_history = draw_step_history(jax.random.fold_in(seeds[11], 71), 0)
    grad_history = draw_grad_history(jax.random.fold_in(seeds[11], 71), 0)
    return {"coords": coords, "anchor": anchor, "atom_types": atom_types, "halo_send": halo_send, "neighbours": neighbours, "live_counts": live_counts, "rep_coef": rep_coef, "disp_coef": disp_coef, "charge": charge, "step_history": step_history, "grad_history": grad_history}


domain_side = 3.0
step_length = 0.5

def export_sizes(atoms_local):
    face_rows = atoms_local // 8
    edge_rows = max(atoms_local // 64, 8)
    corner_rows = max(atoms_local // 512, 8)
    return [face_rows, face_rows, edge_rows, face_rows, edge_rows, edge_rows, corner_rows]

def tile_gradient(ext_pos, ext_par, neighbours, live_counts):
    ext_clusters = ext_pos.shape[1] // 8
    pos_tiles = ext_pos.reshape(3, ext_clusters, 8).transpose(0, 2, 1)
    par_tiles = ext_par.reshape(3, ext_clusters, 8).transpose(0, 2, 1)
    cluster_rows = neighbours.shape[0]
    list_width = neighbours.shape[1]
    block_rows = math.gcd(256, cluster_rows)
    block_count = cluster_rows // block_rows
    atom_rank = jnp.arange(8, dtype=jnp.int32)
    ordered_pair = (atom_rank[:, None] < atom_rank[None, :]).astype(jnp.float32)[:, :, None]
    slot_rank = jnp.tile(jnp.arange(list_width, dtype=jnp.int32), block_rows)

    def one_block(state_pair, block_id):
        gradient, energy = state_pair
        first_row = block_id * block_rows
        listed = lax.dynamic_slice_in_dim(neighbours, first_row, block_rows, 0).reshape(-1)
        live_count = jnp.repeat(lax.dynamic_slice_in_dim(live_counts, first_row, block_rows, 0), list_width)
        home_ids = jnp.repeat(first_row + jnp.arange(block_rows, dtype=jnp.int32), list_width)
        live_mask = (slot_rank < live_count).astype(jnp.float32)
        weight = live_mask[None, None, :] * jnp.where((listed == home_ids)[None, None, :], ordered_pair, 1.0)
        pos_home = jnp.repeat(lax.dynamic_slice_in_dim(pos_tiles, first_row, block_rows, 2), list_width, axis=2)
        par_home = jnp.repeat(lax.dynamic_slice_in_dim(par_tiles, first_row, block_rows, 2), list_width, axis=2)
        pos_other = jnp.take(pos_tiles, listed, axis=2)
        par_other = jnp.take(par_tiles, listed, axis=2)
        offset = pos_home[:, :, None, :] - pos_other[:, None, :, :]
        dist_sq = lax.optimization_barrier(jnp.sum(offset * offset, axis=0))
        inverse = 1.0 / (1.0 + dist_sq)
        repulse = par_home[0][:, None, :] * par_other[0][None, :, :]
        attract = par_home[1][:, None, :] * par_other[1][None, :, :]
        coulomb = par_home[2][:, None, :] * par_other[2][None, :, :]
        root_inv = jnp.sqrt(inverse)
        pair_energy = repulse * inverse * inverse - attract * inverse + coulomb * root_inv
        slope = 2.0 * repulse * inverse - attract + 0.5 * coulomb / root_inv
        factor = -2.0 * weight * slope * inverse * inverse
        push_term = factor[None] * offset
        home_grad = lax.optimization_barrier(jnp.sum(push_term, axis=2)).reshape(3, 8, block_rows, list_width).sum(axis=3)
        other_grad = -lax.optimization_barrier(jnp.sum(push_term, axis=1))
        gradient = gradient.at[:, :, listed].add(other_grad)
        current = lax.dynamic_slice_in_dim(gradient, first_row, block_rows, 2)
        gradient = lax.dynamic_update_slice_in_dim(gradient, current + home_grad, first_row, 2)
        energy = energy + jnp.sum(weight * pair_energy)
        return ((gradient, energy), None)
    initial = (jnp.zeros((3, 8, ext_clusters), jnp.float32), jnp.zeros((), jnp.float32))
    (gradient, energy), unused = lax.scan(one_block, initial, jnp.arange(block_count, dtype=jnp.int32))
    return (gradient.transpose(0, 2, 1).reshape(3, -1), energy)

def reference(coords, anchor, atom_types, halo_send, neighbours, live_counts, rep_coef, disp_coef, charge, step_history, grad_history):
    domain_count = N_GX * N_GY * N_GZ
    atoms_local = coords.shape[1] // domain_count
    size_list = export_sizes(atoms_local)
    start_list = [sum(size_list[:block_pos]) for block_pos in range(7)]
    export_total = sum(size_list)
    type_table = jnp.stack([rep_coef, disp_coef, charge])
    params = jnp.take(type_table, atom_types, axis=1)
    pos_domain = coords.reshape(3, domain_count, atoms_local).transpose(1, 0, 2)
    par_domain = params.reshape(3, domain_count, atoms_local).transpose(1, 0, 2)
    send_rows = halo_send.reshape(domain_count, export_total)
    export_pos = jnp.take_along_axis(pos_domain, send_rows[:, None, :], axis=2)
    export_par = jnp.take_along_axis(par_domain, send_rows[:, None, :], axis=2)
    list_domain = neighbours.reshape(domain_count, -1, neighbours.shape[1])
    count_domain = live_counts.reshape(domain_count, -1)

    def per_domain(returned, domain):
        row_x = domain // (N_GY * N_GZ)
        row_y = domain // N_GZ % N_GY
        row_z = domain % N_GZ
        pieces_pos = [pos_domain[domain]]
        pieces_par = [par_domain[domain]]
        sources = []
        for block_code in range(1, 8):
            step_x = block_code // 4
            step_y = block_code // 2 % 2
            step_z = block_code % 2
            block_start = start_list[block_code - 1]
            block_len = size_list[block_code - 1]
            source = ((row_x + step_x) % N_GX * N_GY + (row_y + step_y) % N_GY) * N_GZ + (row_z + step_z) % N_GZ
            shift_vec = jnp.array([step_x, step_y, step_z], jnp.float32) * domain_side
            pieces_pos.append(export_pos[source][:, block_start:block_start + block_len] + shift_vec[:, None])
            pieces_par.append(export_par[source][:, block_start:block_start + block_len])
            sources.append(source)
        ext_pos = jnp.concatenate(pieces_pos, axis=1)
        ext_par = jnp.concatenate(pieces_par, axis=1)
        gradient, energy = tile_gradient(ext_pos, ext_par, list_domain[domain], count_domain[domain])
        for block_code in range(1, 8):
            block_start = start_list[block_code - 1]
            block_len = size_list[block_code - 1]
            begin = atoms_local + block_start
            returned = returned.at[sources[block_code - 1], :, block_start:block_start + block_len].add(gradient[:, begin:begin + block_len])
        return (returned, (gradient[:, :atoms_local], energy))
    returned, (local_grad, energies) = lax.scan(per_domain, jnp.zeros((domain_count, 3, export_total), jnp.float32), jnp.arange(domain_count, dtype=jnp.int32))
    domain_ids = jnp.arange(domain_count, dtype=jnp.int32)[:, None, None]
    component_ids = jnp.arange(3, dtype=jnp.int32)[None, :, None]
    local_grad = local_grad.at[domain_ids, component_ids, send_rows[:, None, :]].add(returned)
    pair_grad = local_grad.transpose(1, 0, 2).reshape(3, -1)
    displacement = coords - anchor
    gradient = (pair_grad + displacement).reshape(-1)
    energy = (jnp.sum(energies) + 0.5 * jnp.sum(displacement * displacement)) / coords.shape[1]
    memory = step_history.shape[0]
    steps_flat = step_history.reshape(memory, -1)
    diffs_flat = grad_history.reshape(memory, -1)
    inverse_sy = [1.0 / jnp.sum(diffs_flat[hist_id] * steps_flat[hist_id]) for hist_id in range(memory)]
    alphas = [None] * memory
    vector = gradient
    for hist_id in reversed(range(memory)):
        alphas[hist_id] = inverse_sy[hist_id] * jnp.sum(steps_flat[hist_id] * vector)
        vector = vector - alphas[hist_id] * diffs_flat[hist_id]
    scaling = jnp.sum(steps_flat[memory - 1] * diffs_flat[memory - 1]) / jnp.sum(diffs_flat[memory - 1] * diffs_flat[memory - 1])
    vector = scaling * vector
    for hist_id in range(memory):
        beta_term = inverse_sy[hist_id] * jnp.sum(diffs_flat[hist_id] * vector)
        vector = vector + (alphas[hist_id] - beta_term) * steps_flat[hist_id]
    new_coords = coords - step_length * vector.reshape(3, -1)
    return (new_coords, energy)
```

```python
import functools

import jax
import jax.numpy as jnp
from jax import lax
from jax.experimental import pallas as pl
from jax.experimental.pallas import tpu as pltpu
from jax.sharding import PartitionSpec as P

domain_side = 3.0
step_length = 0.5
AXES = ("gx", "gy", "gz")
f32 = jnp.float32
bf16 = jnp.bfloat16
i32 = jnp.int32


def export_sizes(atoms_local):
    face_rows = atoms_local // 8
    edge_rows = max(atoms_local // 64, 8)
    corner_rows = max(atoms_local // 512, 8)
    return face_rows, edge_rows, corner_rows


def shifted(value, axis, steps):
    count = lax.axis_size(axis)
    pairs = [(source, (source + steps) % count) for source in range(count)]
    return lax.ppermute(value, axis, pairs)


def iota(shape, dim):
    return lax.broadcasted_iota(i32, shape, dim)


def split_parts(value, parts):
    pieces = []
    for part in range(parts):
        piece = value.astype(bf16)
        pieces.append(piece)
        if part + 1 < parts:
            value = value - piece.astype(f32)
    return pieces


def join_parts(stacked, rows, parts):
    total = stacked[(parts - 1) * rows :]
    for part in reversed(range(parts - 1)):
        total = total + stacked[part * rows : (part + 1) * rows]
    return total


def dot_nn(left, right):
    return lax.dot_general(left, right, (((1,), (0,)), ((), ())), preferred_element_type=f32)


def dot_nt(left, right):
    return lax.dot_general(left, right, (((1,), (1,)), ((), ())), preferred_element_type=f32)


def one_hot(condition):
    return jnp.where(condition, 1.0, 0.0).astype(bf16)


def slab_order(sizes):
    face, edge, corner = sizes
    return 3 * face, 3 * edge + corner


def reordered_send(send, sizes):
    face, edge, corner = sizes
    lane = iota(send.shape, 1)
    to_front = pltpu.roll(send, send.shape[1] - edge, 1)
    to_back = pltpu.roll(send, face, 1)
    moved = jnp.where(lane < 3 * face, to_front, to_back)
    return jnp.where((lane >= 2 * face) & (lane < 3 * face + edge), moved, send)


def send_one_hot(send_row, first, rows):
    row = iota((rows, send_row.shape[1]), 0) + first
    return one_hot(row == send_row)


def export_kernel(sizes, send_ref, coords_ref, types_ref, rep_ref, disp_ref, charge_ref, step_ref, diff_ref, out_ref, par_ref, data_ref):
    atoms = coords_ref.shape[1]
    ntypes = rep_ref.shape[1]
    kinds = one_hot(types_ref[...] == iota((ntypes, atoms), 0))
    sub = iota((8, ntypes), 0)
    table = jnp.where(sub == 0, rep_ref[...], jnp.where(sub == 1, disp_ref[...], jnp.where(sub == 2, charge_ref[...], 0.0)))
    table = jnp.concatenate(split_parts(table, 3), axis=0)
    params = join_parts(dot_nn(table, kinds), 8, 3)
    par_ref[...] = params
    data_ref[0:3, :] = coords_ref[...]
    data_ref[3:6, :] = params[0:3]
    data_ref[6:8, :] = params[6:8]
    head = data_ref[...]
    hist = jnp.concatenate([step_ref[...].reshape(-1, atoms), diff_ref[...].reshape(-1, atoms)], axis=0)
    rows = hist.shape[0]
    left = jnp.concatenate(split_parts(head, 3) + split_parts(hist, 2), axis=0)
    send = reordered_send(send_ref[...], sizes)
    total = None
    chunk = 256
    for first in range(0, atoms, chunk):
        part = dot_nn(left[:, first : first + chunk], send_one_hot(send, first, chunk))
        total = part if total is None else total + part
    out_ref[0:8, :] = join_parts(total[0:24], 8, 3)
    out_ref[8 : 8 + rows, :] = join_parts(total[24:], rows, 2)


def spread_rows(rows6, lanes):
    keep = (iota((8, lanes), 1) & 7) == iota((8, lanes), 0)
    return jnp.concatenate(
        [jnp.where(keep, jnp.broadcast_to(row, (8, lanes)), 0.0) for row in rows6], axis=0
    )


def cluster_map(atoms, clusters):
    return one_hot((iota((atoms, clusters), 0) >> 3) == iota((atoms, clusters), 1))


def to_clusters(rows6, lanes, clusters):
    spread = spread_rows(rows6, lanes)
    left = jnp.concatenate(split_parts(spread, 3), axis=0)
    return join_parts(dot_nn(left, cluster_map(lanes, clusters)), spread.shape[0], 3)


def to_atoms(tiles, lanes):
    clusters = tiles.shape[1]
    spread = one_hot((iota((clusters, lanes), 1) >> 3) == iota((clusters, lanes), 0))
    wide = dot_nn(jnp.concatenate(split_parts(tiles, 3), axis=0), spread)
    wide = join_parts(wide, tiles.shape[0], 3)
    keep = (iota((8, lanes), 1) & 7) == iota((8, lanes), 0)
    rows = []
    for comp in range(tiles.shape[0] // 8):
        slab = wide[comp * 8 : (comp + 1) * 8]
        rows.append(jnp.sum(jnp.where(keep, slab, 0.0), axis=0, keepdims=True))
    return rows


def lane_sum(value):
    return jnp.sum(value, axis=1, keepdims=True)


def local_kernel(coords_ref, par_ref, neigh_ref, step_ref, diff_ref, tiles_ref, other_ref, gram_ref):
    atoms = coords_ref.shape[1]
    clusters = atoms // 8
    slots = neigh_ref.shape[0]
    rows6 = [coords_ref[c : c + 1, :] for c in range(3)] + [par_ref[c : c + 1, :] for c in range(3)]
    tiles = to_clusters(rows6, atoms, clusters)
    tiles_ref[...] = tiles
    left = jnp.concatenate(split_parts(tiles, 3), axis=0)
    rows = tiles.shape[0]
    for slot in range(slots):
        select = one_hot(iota((clusters, clusters), 0) == neigh_ref[slot : slot + 1, :])
        other_ref[:, slot * clusters : (slot + 1) * clusters] = join_parts(dot_nn(left, select), rows, 3)
    memory = step_ref.shape[1]
    lane = iota((memory, 128), 1)
    sub = iota((memory, 128), 0)
    placed = jnp.zeros((memory, 128), f32)
    for j in range(memory):
        sy = None
        yy = None
        for comp in range(3):
            row = jnp.broadcast_to(diff_ref[comp, j : j + 1, :], (memory, atoms))
            one = step_ref[comp] * row
            two = diff_ref[comp] * row
            sy = one if sy is None else sy + one
            yy = two if yy is None else yy + two
        placed = placed + jnp.where(lane == sub * memory + j, lane_sum(sy), 0.0)
        placed = placed + jnp.where(lane == memory * memory + sub * memory + j, lane_sum(yy), 0.0)
    gram_ref[...] = placed


def remapped(neigh, clusters, sizes):
    face, edge, corner = (size // 8 for size in sizes)
    edge_first = clusters + 2 * face
    shift = jnp.where(
        neigh >= edge_first + edge + face,
        0,
        jnp.where(neigh >= edge_first + edge, -edge, jnp.where(neigh >= edge_first, face, 0)),
    )
    return neigh + shift


def linear_device(offset):
    total = 0
    for axis, step in zip(AXES, offset):
        count = lax.axis_size(axis)
        total = total * count + (lax.axis_index(axis) + step + count) % count
    return total


def code_bits(code):
    return code // 4, code // 2 % 2, code % 2


def pair_kernel(
    sizes, tiles_ref, other_ref, gram_ref, pz_ref, py_ref, px_ref, neigh_ref, live_ref,
    coords_ref, anchor_ref, step_ref, diff_ref,
    chunk_ref, grad_ref,
    select_ref, gather_ref, push_ref,
):
    face, edge, corner = sizes
    atoms = coords_ref.shape[1]
    clusters = atoms // 8
    slots = neigh_ref.shape[0]
    faces, edges = slab_order(sizes)
    lanes = faces + 128
    halo_clusters = 128
    memory = step_ref.shape[1]

    edge_lane = iota((pz_ref.shape[0], 128), 1)
    edge_slab = jnp.where(edge_lane < edge, py_ref[:, face : face + 128], px_ref[:, face : face + 128])
    halo = jnp.concatenate([pz_ref[:, :face], py_ref[:, :face], px_ref[:, :face], edge_slab], axis=1)
    lane = iota((1, lanes), 1)
    in_x = (lane >= 2 * face) & ((lane < faces) | (lane >= faces + edge))
    in_y = ((lane >= face) & (lane < 2 * face)) | ((lane >= faces) & (lane < faces + edge)) | (lane >= faces + 2 * edge)
    in_z = (lane < face) | ((lane >= faces) & (lane < faces + 2 * edge)) | (lane >= faces + 3 * edge)
    rows6 = [halo[c : c + 1] for c in range(6)]
    for c, inside in enumerate((in_x, in_y, in_z)):
        rows6[c] = rows6[c] + jnp.where(inside, domain_side, 0.0)
    rows6 = [jnp.where(lane < faces + edges, row, 0.0) for row in rows6]
    halo_tiles = to_clusters(rows6, lanes, halo_clusters)
    left = jnp.concatenate(split_parts(halo_tiles, 3), axis=0)
    rows = halo_tiles.shape[0]

    neigh = remapped(neigh_ref[...], clusters, sizes)
    for slot in range(slots):
        cols = slice(slot * clusters, (slot + 1) * clusters)
        row = neigh[slot : slot + 1, :]
        select_ref[:, cols] = one_hot(iota((clusters + halo_clusters, clusters), 0) == row)
        far = dot_nn(left, select_ref[clusters:, cols])
        gather_ref[:, cols] = other_ref[:, cols] + join_parts(far, rows, 3)

    rank = iota((8, clusters), 0)
    home_id = iota((8, clusters), 1)
    live = jnp.broadcast_to(live_ref[...], (8, clusters))
    full = []
    half = []
    for slot in range(slots):
        on = jnp.where(live > slot, 1.0, 0.0)
        full.append(on)
        half.append(jnp.where(neigh[slot : slot + 1, :] == home_id, 0.0, on))

    energy = jnp.zeros((8, clusters), f32)
    home_rows = [[None] * 8 for _ in range(3)]
    for p in range(8):
        home = [jnp.broadcast_to(tiles_ref[c * 8 + p : c * 8 + p + 1, :], (8, clusters)) for c in range(6)]
        upper = rank > p
        sums = [jnp.zeros((8, clusters), f32) for _ in range(3)]
        for slot in range(slots):
            cols = slice(slot * clusters, (slot + 1) * clusters)
            other = [gather_ref[c * 8 : (c + 1) * 8, cols] for c in range(6)]
            offset = [home[c] - other[c] for c in range(3)]
            dist_sq = offset[0] * offset[0] + offset[1] * offset[1] + offset[2] * offset[2]
            root = lax.rsqrt(1.0 + dist_sq)
            inverse = root * root
            repulse = home[3] * other[3] * inverse
            attract = home[4] * other[4]
            coulomb = home[5] * other[5] * root
            weight = jnp.where(upper, full[slot], half[slot])
            energy = energy + weight * (inverse * (repulse - attract) + coulomb)
            factor = weight * inverse * (inverse * (4.0 * repulse - 2.0 * attract) + coulomb)
            for c in range(3):
                term = factor * offset[c]
                sums[c] = sums[c] + term
                place = (slice(c * 8, (c + 1) * 8), cols)
                push_ref[place] = term if p == 0 else push_ref[place] + term
        for c in range(3):
            home_rows[c][p] = jnp.sum(sums[c], axis=0, keepdims=True)
    home_grad = jnp.concatenate([home_rows[c][p] for c in range(3) for p in range(8)], axis=0)
    back = jnp.concatenate(split_parts(push_ref[...], 2), axis=0)
    tile_grad = join_parts(dot_nt(back, select_ref[...]), 24, 2)
    own = to_atoms(tile_grad[:, :clusters] - home_grad, atoms)
    returned = to_atoms(tile_grad[:, clusters:], lanes)

    step_dots = jnp.zeros((memory, atoms), f32)
    diff_dots = jnp.zeros((memory, atoms), f32)
    far_step = jnp.zeros((memory, lanes), f32)
    far_diff = jnp.zeros((memory, lanes), f32)
    moved = jnp.zeros((1, atoms), f32)
    slab_lane = iota((memory, lanes), 1)
    for c in range(3):
        displacement = coords_ref[c : c + 1, :] - anchor_ref[c : c + 1, :]
        moved = moved + displacement * displacement
        grad = own[c] + displacement
        grad_ref[c : c + 1, :] = grad
        wide = jnp.broadcast_to(grad, (memory, atoms))
        step_dots = step_dots + step_ref[c] * wide
        diff_dots = diff_dots + diff_ref[c] * wide
        wide = jnp.broadcast_to(returned[c], (memory, lanes))
        far_step = far_step + halo[8 + c * memory : 8 + (c + 1) * memory] * wide
        far_diff = far_diff + halo[8 + (3 + c) * memory : 8 + (4 + c) * memory] * wide
    used = slab_lane < faces + edges
    step_sum = lane_sum(step_dots) + lane_sum(jnp.where(used, far_step, 0.0))
    diff_sum = lane_sum(diff_dots) + lane_sum(jnp.where(used, far_diff, 0.0))
    energy_sum = lane_sum(jnp.sum(energy, axis=0, keepdims=True)) + 0.5 * lane_sum(moved)
    sub = iota((memory, 128), 0)
    lane = iota((memory, 128), 1)
    dots = jnp.where(lane == sub, step_sum, 0.0) + jnp.where(lane == sub + memory, diff_sum, 0.0)
    dots = jnp.sum(dots, axis=0, keepdims=True)
    dots = dots + jnp.where(iota((1, 128), 1) == 2 * memory, energy_sum, 0.0)
    gram = jnp.sum(gram_ref[...], axis=0, keepdims=True)
    sub8 = iota((8, 128), 0)
    common = jnp.where(sub8 == 6, dots, jnp.where(sub8 == 7, gram, 0.0))
    for device in range(chunk_ref.shape[0]):
        chunk_ref[device] = common
    for code in range(1, 8):
        target = linear_device(code_bits(code))
        start = {1: 0, 2: face, 4: 2 * face}.get(code, faces)
        pieces = [returned[c][:, start : start + 128] for c in range(3)]
        if code in (1, 2, 4):
            pieces += [returned[c][:, start + 128 : start + 256] for c in range(3)]
        chunk_ref[target, 0 : len(pieces), :] = jnp.concatenate(pieces, axis=0)


def finish_kernel(sizes, atoms_total, recv_ref, send_ref, grad_ref, coords_ref, step_ref, diff_ref, new_ref, energy_ref):
    face, edge, corner = sizes
    faces, edges = slab_order(sizes)
    atoms = coords_ref.shape[1]
    memory = step_ref.shape[1]
    devices = recv_ref.shape[0]
    total = recv_ref[0]
    for device in range(1, devices):
        total = total + recv_ref[device]
    dots = jnp.broadcast_to(total[6:7, :], (memory, 128))
    gram = jnp.broadcast_to(total[7:8, :], (memory, 128))
    sub = iota((memory, 128), 0)
    lane = iota((memory, 128), 1)

    def pick(row, where):
        return jnp.broadcast_to(lane_sum(jnp.where(where, row, 0.0)), (memory, 128))

    def at(value, m):
        return jnp.broadcast_to(value[m : m + 1, :], (memory, 128))

    step_dots = pick(dots, lane == sub)
    diff_dots = pick(dots, lane == sub + memory)
    energy_ref[...] = lane_sum(jnp.where(iota((1, 128), 1) == 2 * memory, total[6:7, :], 0.0)) / atoms_total
    sy_col = [pick(gram, lane == sub * memory + j) for j in range(memory)]
    sy_row = [pick(gram, lane == j * memory + sub) for j in range(memory)]
    yy_col = [pick(gram, lane == memory * memory + sub * memory + j) for j in range(memory)]
    diagonal = pick(gram, lane == sub * (memory + 1))
    rho = 1.0 / diagonal
    last = memory - 1
    scaling = at(diagonal, last) / at(yy_col[last], last)
    left = step_dots
    alpha = jnp.zeros((memory, 128), f32)
    folded = diff_dots
    for m in reversed(range(memory)):
        value = at(left * rho, m)
        alpha = jnp.where(sub == m, value, alpha)
        left = left - value * sy_col[m]
        folded = folded - value * yy_col[m]
    left = diagonal * alpha - scaling * folded
    coef = jnp.zeros((memory, 128), f32)
    for m in range(memory):
        value = at(left * rho, m)
        coef = jnp.where(sub == m, value, coef)
        left = left - value * sy_row[m]
    diff_coef = -scaling * alpha

    blocks = {code: recv_ref[linear_device(tuple(-bit for bit in code_bits(code)))] for code in range(1, 8)}
    edge_lane = iota((8, 128), 1)
    tail = jnp.where(
        edge_lane < edge,
        blocks[3],
        jnp.where(edge_lane < 2 * edge, blocks[5], jnp.where(edge_lane < 3 * edge, blocks[6], blocks[7])),
    )
    tail = jnp.where(edge_lane < edges, tail, 0.0)
    pieces = []
    for code in (1, 2, 4):
        pieces += [blocks[code][0:3], blocks[code][3:6]]
    pieces.append(tail[0:3])
    returned = jnp.concatenate([jnp.concatenate(pieces, axis=1), jnp.zeros((5, faces + 128), f32)], axis=0)
    back = jnp.concatenate(split_parts(returned, 2), axis=0)
    send = reordered_send(send_ref[...], sizes)
    send = jnp.where(iota(send.shape, 1) < faces + edges, send, -1)
    added = []
    chunk = 256
    for first in range(0, atoms, chunk):
        added.append(join_parts(dot_nt(back, send_one_hot(send, first, chunk)), 8, 2))
    added = jnp.concatenate(added, axis=1)
    widen = atoms // 128
    for c in range(3):
        grad = grad_ref[c : c + 1, :] + added[c : c + 1, :]
        mixed = jnp.tile(coef, (1, widen)) * step_ref[c] + jnp.tile(diff_coef, (1, widen)) * diff_ref[c]
        direction = jnp.tile(scaling[0:1], (1, widen)) * grad + jnp.sum(mixed, axis=0, keepdims=True)
        new_ref[c : c + 1, :] = coords_ref[c : c + 1, :] - step_length * direction


def call(kernel, outs, scratch, *args):
    vmem = pl.BlockSpec(memory_space=pltpu.VMEM)
    return pl.pallas_call(
        kernel,
        out_shape=[jax.ShapeDtypeStruct(shape, dtype) for shape, dtype in outs],
        in_specs=[vmem] * len(args),
        out_specs=[vmem] * len(outs),
        scratch_shapes=scratch,
    )(*args)


def on_device(
    coords,
    anchor,
    atom_types,
    halo_send,
    neighbours,
    live_counts,
    rep_coef,
    disp_coef,
    charge,
    step_history,
    grad_history,
):
    atoms = coords.shape[1]
    clusters = atoms // 8
    memory = step_history.shape[0]
    sizes = export_sizes(atoms)
    face, edge, corner = sizes
    faces, edges = slab_order(sizes)
    lanes = faces + 128
    slots = neighbours.shape[1]
    devices = lax.axis_size("gx") * lax.axis_size("gy") * lax.axis_size("gz")
    assert edges <= 128 and face == 256 and 2 * memory * memory == 128
    steps = step_history.transpose(1, 0, 2)
    diffs = grad_history.transpose(1, 0, 2)
    neigh = neighbours.T
    send = jnp.pad(halo_send, (0, lanes - halo_send.shape[0]), constant_values=-1)[None]
    live = live_counts[None]
    rows = 8 + 6 * memory

    exported, params = call(
        functools.partial(export_kernel, sizes),
        [((rows, lanes), f32), ((8, atoms), f32)],
        [pltpu.VMEM((8, atoms), f32)],
        send, coords, atom_types[None], rep_coef[None], disp_coef[None], charge[None], steps, diffs,
    )
    own_edges = exported[:, faces:]
    edge_lane = lax.broadcasted_iota(i32, own_edges.shape, 1)
    sixes = (edge_lane >= 2 * edge) & (edge_lane < 3 * edge)
    fives = (edge_lane >= edge) & (edge_lane < 2 * edge)
    payload = jnp.concatenate([exported[:, :face], own_edges], axis=1)
    pz = shifted(payload, "gz", -1)
    tiles, other, gram = call(
        local_kernel,
        [((48, clusters), f32), ((48, slots * clusters), f32), ((memory, 128), f32)],
        [],
        coords, params, neigh, steps, diffs,
    )
    payload = jnp.concatenate(
        [exported[:, face : 2 * face], jnp.where(sixes, own_edges, pz[:, face:])], axis=1
    )
    py = shifted(payload, "gy", -1)
    payload = jnp.concatenate(
        [exported[:, 2 * face : faces], jnp.where(fives, pz[:, face:], py[:, face:])], axis=1
    )
    px = shifted(payload, "gx", -1)
    chunks, grad = call(
        functools.partial(pair_kernel, sizes),
        [((devices, 8, 128), f32), ((3, atoms), f32)],
        [
            pltpu.VMEM((clusters + 128, slots * clusters), bf16),
            pltpu.VMEM((48, slots * clusters), f32),
            pltpu.VMEM((24, slots * clusters), f32),
        ],
        tiles, other, gram, pz, py, px, neigh, live, coords, anchor, steps, diffs,
    )
    received = lax.all_to_all(chunks, AXES, 0, 0, tiled=True)
    new_coords, energy = call(
        functools.partial(finish_kernel, sizes, atoms * devices),
        [((3, atoms), f32), ((1, 1), f32)],
        [],
        received, send, grad, coords, steps, diffs,
    )
    return (new_coords, energy[0, 0])


def solution(mesh):
    placed = (
        P(None, AXES),
        P(None, AXES),
        P(AXES),
        P(AXES),
        P(AXES, None),
        P(AXES),
        P(),
        P(),
        P(),
        P(None, None, AXES),
        P(None, None, AXES),
    )
    return jax.shard_map(
        on_device,
        mesh=mesh,
        in_specs=placed,
        out_specs=(P(None, AXES), P()),
        check_vma=False,
    )
```

```python
import functools
import math

import jax
import jax.numpy as jnp
from jax import lax
from jax.experimental import pallas as pl
from jax.experimental.pallas import tpu as pltpu
from jax.sharding import PartitionSpec as P

domain_side = 3.0
step_length = 0.5
AXES = ("gx", "gy", "gz")
f32 = jnp.float32
bf16 = jnp.bfloat16
i32 = jnp.int32


def export_sizes(atoms_local):
    face_rows = atoms_local // 8
    edge_rows = max(atoms_local // 64, 8)
    corner_rows = max(atoms_local // 512, 8)
    return face_rows, edge_rows, corner_rows


def shifted(value, axes, steps):
    shape = [lax.axis_size(axis) for axis in axes]
    pairs = []
    for source in range(math.prod(shape)):
        rest, target, scale = source, 0, 1
        for count in reversed(shape):
            target += (rest % count + steps) % count * scale
            rest //= count
            scale *= count
        pairs.append((source, target))
    return lax.ppermute(value, axes, pairs)


def iota(shape, dim):
    return lax.broadcasted_iota(i32, shape, dim)


def split_parts(value, parts):
    pieces = []
    for part in range(parts):
        piece = value.astype(bf16)
        pieces.append(piece)
        if part + 1 < parts:
            value = value - piece.astype(f32)
    return pieces


def join_parts(stacked, rows, parts):
    total = stacked[(parts - 1) * rows :]
    for part in reversed(range(parts - 1)):
        total = total + stacked[part * rows : (part + 1) * rows]
    return total


def dot_nn(left, right):
    return lax.dot_general(left, right, (((1,), (0,)), ((), ())), preferred_element_type=f32)


def dot_nt(left, right):
    return lax.dot_general(left, right, (((1,), (1,)), ((), ())), preferred_element_type=f32)


def one_hot(condition):
    return jnp.where(condition, 1.0, 0.0).astype(bf16)


def slab_order(sizes):
    face, edge, corner = sizes
    return 3 * face, 3 * edge + corner


def reordered_send(send, sizes):
    face, edge, corner = sizes
    lane = iota(send.shape, 1)
    to_front = pltpu.roll(send, send.shape[1] - edge, 1)
    to_back = pltpu.roll(send, face, 1)
    moved = jnp.where(lane < 3 * face, to_front, to_back)
    return jnp.where((lane >= 2 * face) & (lane < 3 * face + edge), moved, send)


def send_one_hot(send_row, first, rows):
    row = iota((rows, send_row.shape[1]), 0) + first
    return one_hot(row == send_row)


def export_kernel(
    sizes,
    send_hbm, coords_hbm, types_hbm, rep_hbm, disp_hbm, charge_hbm, step_hbm, diff_hbm, anchor_hbm, neigh_hbm, live_hbm,
    pay_z_ref, pay_x_ref, pay_y_ref, pay_e_ref, par_ref, order_ref,
    coords_ref, step_ref, diff_ref, anchor_ref, neigh_ref, live_ref,
    data_ref, send_pad_ref, send_ref, types_ref, rep_ref, disp_ref, charge_ref, arrived,
):
    face, edge, corner = sizes
    faces, edges = slab_order(sizes)
    pairs = [
        (send_hbm, send_ref), (types_hbm, types_ref), (rep_hbm, rep_ref), (disp_hbm, disp_ref),
        (charge_hbm, charge_ref), (coords_hbm, coords_ref), (step_hbm, step_ref), (diff_hbm, diff_ref),
        (anchor_hbm, anchor_ref), (neigh_hbm, neigh_ref), (live_hbm, live_ref),
    ]
    copies = [pltpu.make_async_copy(source, place, arrived.at[k]) for k, (source, place) in enumerate(pairs)]
    for copy in copies:
        copy.start()
    for copy in copies[:6]:
        copy.wait()
    atoms = coords_ref.shape[1]
    ntypes = rep_ref.shape[1]
    send_pad_ref[...] = jnp.full(send_pad_ref.shape, -1, i32)
    count = send_ref.shape[0]
    for first in range(0, count, 128):
        width = min(128, count - first)
        send_pad_ref[:, first : first + width] = send_ref[pl.ds(first, width)].reshape(1, width)
    send = reordered_send(send_pad_ref[:, : faces + 128], sizes)
    order_ref[:, : faces + 128] = send
    kinds = one_hot(types_ref[...] == iota((ntypes, atoms), 0))
    sub = iota((8, ntypes), 0)
    table = jnp.where(sub == 0, rep_ref[...], jnp.where(sub == 1, disp_ref[...], jnp.where(sub == 2, charge_ref[...], 0.0)))
    table = jnp.concatenate(split_parts(table, 3), axis=0)
    params = join_parts(dot_nn(table, kinds), 8, 3)
    par_ref[...] = params
    data_ref[0:3, :] = coords_ref[...]
    data_ref[3:6, :] = params[0:3]
    data_ref[6:8, :] = params[6:8]
    head = data_ref[...]
    for copy in copies[6:]:
        copy.wait()
    hist = jnp.concatenate([step_ref[...].reshape(-1, atoms), diff_ref[...].reshape(-1, atoms)], axis=0)
    rows = hist.shape[0]
    left = jnp.concatenate(split_parts(head, 3) + split_parts(hist, 2), axis=0)
    total = None
    chunk = 256
    for first in range(0, atoms, chunk):
        part = dot_nn(left[:, first : first + chunk], send_one_hot(send, first, chunk))
        total = part if total is None else total + part
    out = jnp.concatenate([join_parts(total[0:24], 8, 3), join_parts(total[24:], rows, 2)], axis=0)
    pay_e_ref[...] = out[:, faces:]
    for ref, first in ((pay_z_ref, 0), (pay_y_ref, face), (pay_x_ref, 2 * face)):
        ref[:, :face] = out[:, first : first + face]
        ref[:, face:] = out[:, faces:]


def spread_rows(rows6, lanes):
    keep = (iota((8, lanes), 1) & 7) == iota((8, lanes), 0)
    return jnp.concatenate(
        [jnp.where(keep, jnp.broadcast_to(row, (8, lanes)), 0.0) for row in rows6], axis=0
    )


def cluster_map(atoms, clusters):
    return one_hot((iota((atoms, clusters), 0) >> 3) == iota((atoms, clusters), 1))


def to_clusters(rows6, lanes, clusters):
    spread = spread_rows(rows6, lanes)
    left = jnp.concatenate(split_parts(spread, 3), axis=0)
    return join_parts(dot_nn(left, cluster_map(lanes, clusters)), spread.shape[0], 3)


def to_atoms(tiles, lanes):
    clusters = tiles.shape[1]
    spread = one_hot((iota((clusters, lanes), 1) >> 3) == iota((clusters, lanes), 0))
    wide = dot_nn(jnp.concatenate(split_parts(tiles, 3), axis=0), spread)
    wide = join_parts(wide, tiles.shape[0], 3)
    keep = (iota((8, lanes), 1) & 7) == iota((8, lanes), 0)
    rows = []
    for comp in range(tiles.shape[0] // 8):
        slab = wide[comp * 8 : (comp + 1) * 8]
        rows.append(jnp.sum(jnp.where(keep, slab, 0.0), axis=0, keepdims=True))
    return rows


def lane_sum(value):
    return jnp.sum(value, axis=1, keepdims=True)


def local_kernel(coords_ref, par_ref, neigh_ref, tiles_ref, other_ref):
    atoms = coords_ref.shape[1]
    clusters = atoms // 8
    slots = neigh_ref.shape[0]
    rows6 = [coords_ref[c : c + 1, :] for c in range(3)] + [par_ref[c : c + 1, :] for c in range(3)]
    tiles = to_clusters(rows6, atoms, clusters)
    tiles_ref[...] = tiles
    left = jnp.concatenate(split_parts(tiles, 3), axis=0)
    rows = tiles.shape[0]
    for slot in range(slots):
        select = one_hot(iota((clusters, clusters), 0) == neigh_ref[slot : slot + 1, :])
        other_ref[:, slot * clusters : (slot + 1) * clusters] = join_parts(dot_nn(left, select), rows, 3)


def gram_kernel(step_ref, diff_ref, gram_ref):
    memory, atoms = step_ref.shape[1:]
    lane = iota((memory, 128), 1)
    sub = iota((memory, 128), 0)
    placed = jnp.zeros((memory, 128), f32)
    for j in range(memory):
        sy = None
        yy = None
        for comp in range(3):
            row = jnp.broadcast_to(diff_ref[comp, j : j + 1, :], (memory, atoms))
            one = step_ref[comp] * row
            two = diff_ref[comp] * row
            sy = one if sy is None else sy + one
            yy = two if yy is None else yy + two
        placed = placed + jnp.where(lane == sub * memory + j, lane_sum(sy), 0.0)
        placed = placed + jnp.where(lane == memory * memory + sub * memory + j, lane_sum(yy), 0.0)
    gram_ref[...] = placed


def merge_kernel(sizes, pay_ref, pz_ref, px_ref, pe_ref, out_ref):
    face, edge, corner = sizes
    lane = iota((pay_ref.shape[0], 128), 1)
    slab = jnp.where(
        lane < edge,
        pz_ref[:, face:],
        jnp.where((lane >= 2 * edge) & (lane < 3 * edge), px_ref[:, face:], pe_ref[...]),
    )
    out_ref[:, :face] = pay_ref[:, :face]
    out_ref[:, face:] = slab


def remapped(neigh, clusters, sizes):
    face, edge, corner = (size // 8 for size in sizes)
    edge_first = clusters + 2 * face
    shift = jnp.where(
        neigh >= edge_first + edge + face,
        0,
        jnp.where(neigh >= edge_first + edge, -edge, jnp.where(neigh >= edge_first, face, 0)),
    )
    return neigh + shift


def linear_device(offset):
    total = 0
    for axis, step in zip(AXES, offset):
        count = lax.axis_size(axis)
        total = total * count + (lax.axis_index(axis) + step + count) % count
    return total


def code_bits(code):
    return code // 4, code // 2 % 2, code % 2


def pair_kernel(
    sizes, tiles_ref, other_ref, gram_ref, pz_ref, py_ref, px_ref, pe_ref, neigh_ref, live_ref,
    coords_ref, anchor_ref, step_ref, diff_ref,
    chunk_ref, grad_ref,
    select_ref, gather_ref, push_ref,
):
    face, edge, corner = sizes
    atoms = coords_ref.shape[1]
    clusters = atoms // 8
    slots = neigh_ref.shape[0]
    faces, edges = slab_order(sizes)
    lanes = faces + 128
    halo_clusters = 128
    memory = step_ref.shape[1]

    edge_lane = iota((pz_ref.shape[0], 128), 1)
    edge_slab = jnp.where((edge_lane >= edge) & (edge_lane < 2 * edge), pe_ref[...], py_ref[:, face:])
    halo = jnp.concatenate([pz_ref[:, :face], py_ref[:, :face], px_ref[:, :face], edge_slab], axis=1)
    lane = iota((1, lanes), 1)
    in_x = (lane >= 2 * face) & ((lane < faces) | (lane >= faces + edge))
    in_y = ((lane >= face) & (lane < 2 * face)) | ((lane >= faces) & (lane < faces + edge)) | (lane >= faces + 2 * edge)
    in_z = (lane < face) | ((lane >= faces) & (lane < faces + 2 * edge)) | (lane >= faces + 3 * edge)
    rows6 = [halo[c : c + 1] for c in range(6)]
    for c, inside in enumerate((in_x, in_y, in_z)):
        rows6[c] = rows6[c] + jnp.where(inside, domain_side, 0.0)
    rows6 = [jnp.where(lane < faces + edges, row, 0.0) for row in rows6]
    halo_tiles = to_clusters(rows6, lanes, halo_clusters)
    left = jnp.concatenate(split_parts(halo_tiles, 3), axis=0)
    rows = halo_tiles.shape[0]

    neigh = remapped(neigh_ref[...], clusters, sizes)
    for slot in range(slots):
        cols = slice(slot * clusters, (slot + 1) * clusters)
        row = neigh[slot : slot + 1, :]
        select_ref[:, cols] = one_hot(iota((clusters + halo_clusters, clusters), 0) == row)
        far = dot_nn(left, select_ref[clusters:, cols])
        gather_ref[:, cols] = other_ref[:, cols] + join_parts(far, rows, 3)

    rank = iota((8, clusters), 0)
    home_id = iota((8, clusters), 1)
    live = jnp.broadcast_to(live_ref[...], (8, clusters))
    full = []
    half = []
    for slot in range(slots):
        on = jnp.where(live > slot, 1.0, 0.0)
        full.append(on)
        half.append(jnp.where(neigh[slot : slot + 1, :] == home_id, 0.0, on))

    energy = jnp.zeros((8, clusters), f32)
    home_rows = [[None] * 8 for _ in range(3)]
    for p in range(8):
        home = [jnp.broadcast_to(tiles_ref[c * 8 + p : c * 8 + p + 1, :], (8, clusters)) for c in range(6)]
        upper = rank > p
        sums = [jnp.zeros((8, clusters), f32) for _ in range(3)]
        for slot in range(slots):
            cols = slice(slot * clusters, (slot + 1) * clusters)
            other = [gather_ref[c * 8 : (c + 1) * 8, cols] for c in range(6)]
            offset = [home[c] - other[c] for c in range(3)]
            dist_sq = offset[0] * offset[0] + offset[1] * offset[1] + offset[2] * offset[2]
            root = lax.rsqrt(1.0 + dist_sq)
            inverse = root * root
            repulse = home[3] * other[3] * inverse
            attract = home[4] * other[4]
            coulomb = home[5] * other[5] * root
            weight = jnp.where(upper, full[slot], half[slot])
            energy = energy + weight * (inverse * (repulse - attract) + coulomb)
            factor = weight * inverse * (inverse * (4.0 * repulse - 2.0 * attract) + coulomb)
            for c in range(3):
                term = factor * offset[c]
                sums[c] = sums[c] + term
                place = (slice(c * 8, (c + 1) * 8), cols)
                push_ref[place] = term if p == 0 else push_ref[place] + term
        for c in range(3):
            home_rows[c][p] = jnp.sum(sums[c], axis=0, keepdims=True)
    home_grad = jnp.concatenate([home_rows[c][p] for c in range(3) for p in range(8)], axis=0)
    back = jnp.concatenate(split_parts(push_ref[...], 2), axis=0)
    tile_grad = join_parts(dot_nt(back, select_ref[...]), 24, 2)
    own = to_atoms(tile_grad[:, :clusters] - home_grad, atoms)
    returned = to_atoms(tile_grad[:, clusters:], lanes)

    step_dots = jnp.zeros((memory, atoms), f32)
    diff_dots = jnp.zeros((memory, atoms), f32)
    far_step = jnp.zeros((memory, lanes), f32)
    far_diff = jnp.zeros((memory, lanes), f32)
    moved = jnp.zeros((1, atoms), f32)
    slab_lane = iota((memory, lanes), 1)
    for c in range(3):
        displacement = coords_ref[c : c + 1, :] - anchor_ref[c : c + 1, :]
        moved = moved + displacement * displacement
        grad = own[c] + displacement
        grad_ref[c : c + 1, :] = grad
        wide = jnp.broadcast_to(grad, (memory, atoms))
        step_dots = step_dots + step_ref[c] * wide
        diff_dots = diff_dots + diff_ref[c] * wide
        wide = jnp.broadcast_to(returned[c], (memory, lanes))
        far_step = far_step + halo[8 + c * memory : 8 + (c + 1) * memory] * wide
        far_diff = far_diff + halo[8 + (3 + c) * memory : 8 + (4 + c) * memory] * wide
    used = slab_lane < faces + edges
    step_sum = lane_sum(step_dots) + lane_sum(jnp.where(used, far_step, 0.0))
    diff_sum = lane_sum(diff_dots) + lane_sum(jnp.where(used, far_diff, 0.0))
    energy_sum = lane_sum(jnp.sum(energy, axis=0, keepdims=True)) + 0.5 * lane_sum(moved)
    sub = iota((memory, 128), 0)
    lane = iota((memory, 128), 1)
    dots = jnp.where(lane == sub, step_sum, 0.0) + jnp.where(lane == sub + memory, diff_sum, 0.0)
    dots = jnp.sum(dots, axis=0, keepdims=True)
    dots = dots + jnp.where(iota((1, 128), 1) == 2 * memory, energy_sum, 0.0)
    gram = jnp.sum(gram_ref[...], axis=0, keepdims=True)
    sub8 = iota((8, 128), 0)
    common = jnp.where(sub8 == 6, dots, jnp.where(sub8 == 7, gram, 0.0))
    for device in range(chunk_ref.shape[0]):
        chunk_ref[device] = common
    for code in range(1, 8):
        target = linear_device(code_bits(code))
        start = {1: 0, 2: face, 4: 2 * face}.get(code, faces)
        pieces = [returned[c][:, start : start + 128] for c in range(3)]
        if code in (1, 2, 4):
            pieces += [returned[c][:, start + 128 : start + 256] for c in range(3)]
        chunk_ref[target, 0 : len(pieces), :] = jnp.concatenate(pieces, axis=0)


def finish_kernel(sizes, atoms_total, recv_ref, send_ref, grad_ref, coords_ref, step_ref, diff_ref, new_ref, energy_ref):
    face, edge, corner = sizes
    faces, edges = slab_order(sizes)
    atoms = coords_ref.shape[1]
    memory = step_ref.shape[1]
    devices = recv_ref.shape[0]
    total = recv_ref[0]
    for device in range(1, devices):
        total = total + recv_ref[device]
    dots = jnp.broadcast_to(total[6:7, :], (memory, 128))
    gram = jnp.broadcast_to(total[7:8, :], (memory, 128))
    sub = iota((memory, 128), 0)
    lane = iota((memory, 128), 1)

    def pick(row, where):
        return jnp.broadcast_to(lane_sum(jnp.where(where, row, 0.0)), (memory, 128))

    def at(value, m):
        return jnp.broadcast_to(value[m : m + 1, :], (memory, 128))

    step_dots = pick(dots, lane == sub)
    diff_dots = pick(dots, lane == sub + memory)
    energy_ref[...] = lane_sum(jnp.where(iota((1, 128), 1) == 2 * memory, total[6:7, :], 0.0)) / atoms_total
    sy_col = [pick(gram, lane == sub * memory + j) for j in range(memory)]
    sy_row = [pick(gram, lane == j * memory + sub) for j in range(memory)]
    yy_col = [pick(gram, lane == memory * memory + sub * memory + j) for j in range(memory)]
    diagonal = pick(gram, lane == sub * (memory + 1))
    rho = 1.0 / diagonal
    last = memory - 1
    scaling = at(diagonal, last) / at(yy_col[last], last)
    left = step_dots
    alpha = jnp.zeros((memory, 128), f32)
    folded = diff_dots
    for m in reversed(range(memory)):
        value = at(left * rho, m)
        alpha = jnp.where(sub == m, value, alpha)
        left = left - value * sy_col[m]
        folded = folded - value * yy_col[m]
    left = diagonal * alpha - scaling * folded
    coef = jnp.zeros((memory, 128), f32)
    for m in range(memory):
        value = at(left * rho, m)
        coef = jnp.where(sub == m, value, coef)
        left = left - value * sy_row[m]
    diff_coef = -scaling * alpha

    blocks = {code: recv_ref[linear_device(tuple(-bit for bit in code_bits(code)))] for code in range(1, 8)}
    edge_lane = iota((8, 128), 1)
    tail = jnp.where(
        edge_lane < edge,
        blocks[3],
        jnp.where(edge_lane < 2 * edge, blocks[5], jnp.where(edge_lane < 3 * edge, blocks[6], blocks[7])),
    )
    tail = jnp.where(edge_lane < edges, tail, 0.0)
    pieces = []
    for code in (1, 2, 4):
        pieces += [blocks[code][0:3], blocks[code][3:6]]
    pieces.append(tail[0:3])
    returned = jnp.concatenate([jnp.concatenate(pieces, axis=1), jnp.zeros((5, faces + 128), f32)], axis=0)
    back = jnp.concatenate(split_parts(returned, 2), axis=0)
    send = send_ref[:, : faces + 128]
    added = []
    chunk = 256
    for first in range(0, atoms, chunk):
        added.append(join_parts(dot_nt(back, send_one_hot(send, first, chunk)), 8, 2))
    added = jnp.concatenate(added, axis=1)
    widen = atoms // 128
    for c in range(3):
        grad = grad_ref[c : c + 1, :] + added[c : c + 1, :]
        mixed = jnp.tile(coef, (1, widen)) * step_ref[c] + jnp.tile(diff_coef, (1, widen)) * diff_ref[c]
        direction = jnp.tile(scaling[0:1], (1, widen)) * grad + jnp.sum(mixed, axis=0, keepdims=True)
        new_ref[c : c + 1, :] = coords_ref[c : c + 1, :] - step_length * direction


def call(kernel, outs, scratch, *args, limit_mib=16, space=pltpu.VMEM):
    if space == pltpu.HBM:
        args = [pltpu.with_memory_space_constraint(arg, pltpu.HBM) for arg in args]
    return pl.pallas_call(
        kernel,
        out_shape=[jax.ShapeDtypeStruct(shape, dtype) for shape, dtype in outs],
        in_specs=[pl.BlockSpec(memory_space=space)] * len(args),
        out_specs=[pl.BlockSpec(memory_space=pltpu.VMEM)] * len(outs),
        scratch_shapes=scratch,
        compiler_params=pltpu.CompilerParams(vmem_limit_bytes=limit_mib << 20),
    )(*args)


def on_device(
    coords,
    anchor,
    atom_types,
    halo_send,
    neighbours,
    live_counts,
    rep_coef,
    disp_coef,
    charge,
    step_history,
    grad_history,
):
    atoms = coords.shape[1]
    clusters = atoms // 8
    memory = step_history.shape[0]
    sizes = export_sizes(atoms)
    face, edge, corner = sizes
    faces, edges = slab_order(sizes)
    lanes = faces + 128
    wide = pl.cdiv(lanes, 1024) * 1024
    slots = neighbours.shape[1]
    devices = lax.axis_size("gx") * lax.axis_size("gy") * lax.axis_size("gz")
    assert edges <= 128 and face == 256 and 2 * memory * memory == 128
    steps = step_history.transpose(1, 0, 2)
    diffs = grad_history.transpose(1, 0, 2)
    neigh = neighbours.T
    live = live_counts[None]
    rows = 8 + 6 * memory

    ntypes = rep_coef.shape[0]
    pay_z, pay_x, pay_y, pay_e, params, order, coords_v, steps_v, diffs_v, anchor_v, neigh_v, live_v = call(
        functools.partial(export_kernel, sizes),
        [((rows, face + 128), f32)] * 3
        + [((rows, 128), f32), ((8, atoms), f32), ((1, wide), i32)]
        + [(value.shape, value.dtype) for value in (coords, steps, diffs, anchor, neigh, live)],
        [
            pltpu.VMEM((8, atoms), f32),
            pltpu.VMEM((1, wide), i32),
            pltpu.VMEM(halo_send.shape, i32),
            pltpu.VMEM((1, atoms), i32),
            pltpu.VMEM((1, ntypes), f32),
            pltpu.VMEM((1, ntypes), f32),
            pltpu.VMEM((1, ntypes), f32),
            pltpu.SemaphoreType.DMA((11,)),
        ],
        halo_send, coords, atom_types[None], rep_coef[None], disp_coef[None], charge[None],
        steps, diffs, anchor, neigh, live,
        space=pltpu.HBM,
    )
    px = shifted(pay_x, ("gx",), -1)
    pe = shifted(pay_e, ("gx", "gz"), -1)
    pz = shifted(pay_z, ("gz",), -1)
    tiles, other = call(
        local_kernel,
        [((48, clusters), f32), ((48, slots * clusters), f32)],
        [],
        coords_v, params, neigh_v,
    )
    pay_y, tiles = lax.optimization_barrier((pay_y, tiles))
    (pay_y,) = call(
        functools.partial(merge_kernel, sizes), [((rows, face + 128), f32)], [], pay_y, pz, px, pe, limit_mib=4
    )
    py = shifted(pay_y, ("gy",), -1)
    (gram,) = call(gram_kernel, [((memory, 128), f32)], [], steps_v, diffs_v, limit_mib=8)
    chunks, grad = call(
        functools.partial(pair_kernel, sizes),
        [((devices, 8, 128), f32), ((3, atoms), f32)],
        [
            pltpu.VMEM((clusters + 128, slots * clusters), bf16),
            pltpu.VMEM((48, slots * clusters), f32),
            pltpu.VMEM((24, slots * clusters), f32),
        ],
        tiles, other, gram, pz, py, px, pe, neigh_v, live_v, coords_v, anchor_v, steps_v, diffs_v,
        limit_mib=24,
    )
    received = lax.all_to_all(chunks, AXES, 0, 0, tiled=True)
    new_coords, energy = call(
        functools.partial(finish_kernel, sizes, atoms * devices),
        [((3, atoms), f32), ((1, 1), f32)],
        [],
        received, order, grad, coords_v, steps_v, diffs_v,
    )
    return (new_coords, energy[0, 0])


def solution(mesh):
    placed = (
        P(None, AXES),
        P(None, AXES),
        P(AXES),
        P(AXES),
        P(AXES, None),
        P(AXES),
        P(),
        P(),
        P(),
        P(None, None, AXES),
        P(None, None, AXES),
    )
    return jax.shard_map(
        on_device,
        mesh=mesh,
        in_specs=placed,
        out_specs=(P(None, AXES), P()),
        check_vma=False,
    )
```

```python
import functools
import math

import jax
import jax.numpy as jnp
from jax import lax
from jax.experimental import pallas as pl
from jax.experimental.pallas import tpu as pltpu
from jax.sharding import PartitionSpec as P


domain_side = 3.0
step_length = 0.5
AXES = ("gx", "gy", "gz")
f32 = jnp.float32
bf16 = jnp.bfloat16
i32 = jnp.int32


def export_sizes(atoms_local):
    face_rows = atoms_local // 8
    edge_rows = max(atoms_local // 64, 8)
    corner_rows = max(atoms_local // 512, 8)
    return face_rows, edge_rows, corner_rows


def shifted(value, axes, steps):
    shape = [lax.axis_size(axis) for axis in axes]
    pairs = []
    for source in range(math.prod(shape)):
        rest, target, scale = source, 0, 1
        for count in reversed(shape):
            target += (rest % count + steps) % count * scale
            rest //= count
            scale *= count
        pairs.append((source, target))
    return lax.ppermute(value, axes, pairs)


def iota(shape, dim):
    return lax.broadcasted_iota(i32, shape, dim)


def split_parts(value, parts):
    pieces = []
    for part in range(parts):
        piece = value.astype(bf16)
        pieces.append(piece)
        if part + 1 < parts:
            value = value - piece.astype(f32)
    return pieces


def join_parts(stacked, rows, parts):
    total = stacked[(parts - 1) * rows :]
    for part in reversed(range(parts - 1)):
        total = total + stacked[part * rows : (part + 1) * rows]
    return total


def dot_nn(left, right):
    return lax.dot_general(left, right, (((1,), (0,)), ((), ())), preferred_element_type=f32)


def dot_nt(left, right):
    return lax.dot_general(left, right, (((1,), (1,)), ((), ())), preferred_element_type=f32)


def one_hot(condition):
    return jnp.where(condition, 1.0, 0.0).astype(bf16)


def slab_order(sizes):
    face, edge, corner = sizes
    return 3 * face, 3 * edge + corner


def reordered_send(send, sizes):
    face, edge, _ = sizes
    lane = iota(send.shape, 1)
    to_front = pltpu.roll(send, send.shape[1] - edge, 1)
    to_back = pltpu.roll(send, face, 1)
    moved = jnp.where(lane < 3 * face, to_front, to_back)
    return jnp.where((lane >= 2 * face) & (lane < 3 * face + edge), moved, send)


def send_one_hot(send_row, first, rows):
    row = iota((rows, send_row.shape[1]), 0) + first
    return one_hot(row == send_row)


def export_kernel(
    sizes,
    send_hbm, coords_hbm, types_hbm, rep_hbm, disp_hbm, charge_hbm, step_hbm, diff_hbm, anchor_hbm, neigh_hbm, live_hbm,
    pay_z_ref, pay_y_ref, pay_x_ref, pay_e_ref,
    far_z_ref, far_y_ref, far_x_ref,
    par_ref, order_ref,
    coords_ref, step_ref, diff_ref, anchor_ref, neigh_ref, live_ref,
    data_ref, send_pad_ref, send_ref, types_ref, rep_ref, disp_ref, charge_ref, arrived,
):
    face, edge, _ = sizes
    faces, _ = slab_order(sizes)
    pairs = [
        (send_hbm, send_ref), (types_hbm, types_ref), (rep_hbm, rep_ref), (disp_hbm, disp_ref),
        (charge_hbm, charge_ref), (coords_hbm, coords_ref), (step_hbm, step_ref), (diff_hbm, diff_ref),
        (anchor_hbm, anchor_ref), (neigh_hbm, neigh_ref), (live_hbm, live_ref),
    ]
    copies = [pltpu.make_async_copy(source, place, arrived.at[k]) for k, (source, place) in enumerate(pairs)]
    for copy in copies:
        copy.start()
    for copy in copies[:6]:
        copy.wait()
    atoms = coords_ref.shape[1]
    ntypes = rep_ref.shape[1]
    send_pad_ref[...] = jnp.full(send_pad_ref.shape, -1, i32)
    count = send_ref.shape[0]
    for first in range(0, count, 128):
        width = min(128, count - first)
        send_pad_ref[:, first : first + width] = send_ref[pl.ds(first, width)].reshape(1, width)
    send = reordered_send(send_pad_ref[:, : faces + 128], sizes)
    order_ref[:, : faces + 128] = send
    kinds = one_hot(types_ref[...] == iota((ntypes, atoms), 0))
    sub = iota((8, ntypes), 0)
    table = jnp.where(sub == 0, rep_ref[...], jnp.where(sub == 1, disp_ref[...], jnp.where(sub == 2, charge_ref[...], 0.0)))
    table = jnp.concatenate(split_parts(table, 3), axis=0)
    params = join_parts(dot_nn(table, kinds), 8, 3)
    par_ref[...] = params
    data_ref[0:3, :] = coords_ref[...]
    data_ref[3:6, :] = params[0:3]
    data_ref[6:8, :] = params[6:8]
    head = data_ref[...]
    for copy in copies[6:]:
        copy.wait()
    hist = jnp.concatenate([step_ref[...].reshape(-1, atoms), diff_ref[...].reshape(-1, atoms)], axis=0)
    rows = hist.shape[0]
    left = jnp.concatenate(split_parts(head, 3) + split_parts(hist, 2), axis=0)
    total = None
    chunk = 256
    for first in range(0, atoms, chunk):
        part = dot_nn(left[:, first : first + chunk], send_one_hot(send, first, chunk))
        total = part if total is None else total + part
    head = join_parts(total[0:24], 8, 3)
    hist = join_parts(total[24:], rows, 2)
    tail = jnp.concatenate([head[:, faces:], hist[:, faces:], jnp.zeros((8, 128), f32)], axis=0)
    packs = [packed_slab(tail, place, edge) for place in range(4)]
    for place, (ref, pack) in enumerate(((pay_z_ref, 1), (pay_y_ref, 2), (pay_x_ref, None))):
        ref[0:8, :] = head[:, place * face : place * face + 128]
        ref[8:16, :] = head[:, place * face + 128 : (place + 1) * face]
        if pack is not None:
            ref[16:32, :] = packs[pack]
    pay_e_ref[0:16, :] = packs[0]
    pay_e_ref[16:32, :] = packs[3]
    for place, ref in enumerate((far_z_ref, far_y_ref, far_x_ref)):
        ref[...] = hist[:, place * face : (place + 1) * face]


def packed_slab(tail, place, edge):
    group = iota((16, 128), 1) // edge
    packed = jnp.zeros((16, 128), f32)
    for k in range(4):
        turned = pltpu.roll(tail[16 * k : 16 * k + 16], (k - place) % 4 * edge, 1)
        packed = jnp.where(group == k, turned, packed)
    return packed


def spread_rows(rows6, lanes):
    keep = (iota((8, lanes), 1) & 7) == iota((8, lanes), 0)
    return jnp.concatenate(
        [jnp.where(keep, jnp.broadcast_to(row, (8, lanes)), 0.0) for row in rows6], axis=0
    )


def cluster_map(atoms, clusters):
    return one_hot((iota((atoms, clusters), 0) >> 3) == iota((atoms, clusters), 1))


def to_clusters(rows6, lanes, clusters):
    spread = spread_rows(rows6, lanes)
    left = jnp.concatenate(split_parts(spread, 3), axis=0)
    return join_parts(dot_nn(left, cluster_map(lanes, clusters)), spread.shape[0], 3)


def to_atoms(tiles, lanes):
    clusters = tiles.shape[1]
    spread = one_hot((iota((clusters, lanes), 1) >> 3) == iota((clusters, lanes), 0))
    wide = dot_nn(jnp.concatenate(split_parts(tiles, 3), axis=0), spread)
    wide = join_parts(wide, tiles.shape[0], 3)
    keep = (iota((8, lanes), 1) & 7) == iota((8, lanes), 0)
    rows = []
    for comp in range(tiles.shape[0] // 8):
        slab = wide[comp * 8 : (comp + 1) * 8]
        rows.append(jnp.sum(jnp.where(keep, slab, 0.0), axis=0, keepdims=True))
    return rows


def lane_sum(value):
    return jnp.sum(value, axis=1, keepdims=True)


def local_kernel(coords_ref, par_ref, neigh_ref, tiles_ref, other_ref):
    atoms = coords_ref.shape[1]
    clusters = atoms // 8
    slots = neigh_ref.shape[0]
    rows6 = [coords_ref[c : c + 1, :] for c in range(3)] + [par_ref[c : c + 1, :] for c in range(3)]
    tiles = to_clusters(rows6, atoms, clusters)
    tiles_ref[...] = tiles
    left = jnp.concatenate(split_parts(tiles, 3), axis=0)
    rows = tiles.shape[0]
    for slot in range(slots):
        select = one_hot(iota((clusters, clusters), 0) == neigh_ref[slot : slot + 1, :])
        other_ref[:, slot * clusters : (slot + 1) * clusters] = join_parts(dot_nn(left, select), rows, 3)


def gram_kernel(step_ref, diff_ref, gram_ref):
    memory, atoms = step_ref.shape[1:]
    lane = iota((memory, 128), 1)
    sub = iota((memory, 128), 0)
    placed = jnp.zeros((memory, 128), f32)
    for j in range(memory):
        sy = None
        yy = None
        for comp in range(3):
            row = jnp.broadcast_to(diff_ref[comp, j : j + 1, :], (memory, atoms))
            one = step_ref[comp] * row
            two = diff_ref[comp] * row
            sy = one if sy is None else sy + one
            yy = two if yy is None else yy + two
        placed = placed + jnp.where(lane == sub * memory + j, lane_sum(sy), 0.0)
        placed = placed + jnp.where(lane == memory * memory + sub * memory + j, lane_sum(yy), 0.0)
    gram_ref[...] = placed


def merge_kernel(pay_ref, pz_ref, py_ref, pe_ref, out_ref):
    out_ref[0:16, :] = pay_ref[...]
    out_ref[16:32, :] = pz_ref[16:32, :]
    out_ref[32:48, :] = py_ref[16:32, :]
    out_ref[48:64, :] = pe_ref[16:32, :]


def remapped(neigh, clusters, sizes):
    face, edge, _ = (size // 8 for size in sizes)
    edge_first = clusters + 2 * face
    shift = jnp.where(
        neigh >= edge_first + edge + face,
        0,
        jnp.where(neigh >= edge_first + edge, -edge, jnp.where(neigh >= edge_first, face, 0)),
    )
    return neigh + shift


def linear_device(offset):
    total = 0
    for axis, step in zip(AXES, offset):
        count = lax.axis_size(axis)
        total = total * count + (lax.axis_index(axis) + step + count) % count
    return total


def code_bits(code):
    return code // 4, code // 2 % 2, code % 2


def pair_kernel(
    sizes, tiles_ref, other_ref, gram_ref, pz_ref, py_ref, px_ref, pe_ref, neigh_ref, live_ref,
    coords_ref, anchor_ref, step_ref, diff_ref,
    grad_ref, returned_ref, common_ref,
    select_ref, gather_ref, push_ref,
):
    face, edge, _ = sizes
    atoms = coords_ref.shape[1]
    clusters = atoms // 8
    slots = neigh_ref.shape[0]
    faces, edges = slab_order(sizes)
    lanes = faces + 128
    halo_clusters = 128
    memory = step_ref.shape[1]

    group = iota((8, 128), 1) // edge
    tail = jnp.where(
        group == 0,
        pe_ref[0:8, :],
        jnp.where(
            group == 1,
            pltpu.roll(px_ref[16:24, :], edge, 1),
            jnp.where(group == 2, pltpu.roll(px_ref[32:40, :], 2 * edge, 1), pltpu.roll(px_ref[48:56, :], 3 * edge, 1)),
        ),
    )
    halves = [ref[first : first + 8, :] for ref in (pz_ref, py_ref, px_ref) for first in (0, 8)]
    halo = jnp.concatenate(halves + [tail], axis=1)
    lane = iota((1, lanes), 1)
    in_x = (lane >= 2 * face) & ((lane < faces) | (lane >= faces + edge))
    in_y = ((lane >= face) & (lane < 2 * face)) | ((lane >= faces) & (lane < faces + edge)) | (lane >= faces + 2 * edge)
    in_z = (lane < face) | ((lane >= faces) & (lane < faces + 2 * edge)) | (lane >= faces + 3 * edge)
    rows6 = [halo[c : c + 1] for c in range(6)]
    for c, inside in enumerate((in_x, in_y, in_z)):
        rows6[c] = rows6[c] + jnp.where(inside, domain_side, 0.0)
    rows6 = [jnp.where(lane < faces + edges, row, 0.0) for row in rows6]
    halo_tiles = to_clusters(rows6, lanes, halo_clusters)
    left = jnp.concatenate(split_parts(halo_tiles, 3), axis=0)
    rows = halo_tiles.shape[0]

    neigh = remapped(neigh_ref[...], clusters, sizes)
    for slot in range(slots):
        cols = slice(slot * clusters, (slot + 1) * clusters)
        row = neigh[slot : slot + 1, :]
        select_ref[:, cols] = one_hot(iota((clusters + halo_clusters, clusters), 0) == row)
        far = dot_nn(left, select_ref[clusters:, cols])
        gather_ref[:, cols] = other_ref[:, cols] + join_parts(far, rows, 3)

    rank = iota((8, clusters), 0)
    home_id = iota((8, clusters), 1)
    live = jnp.broadcast_to(live_ref[...], (8, clusters))
    full = []
    half = []
    for slot in range(slots):
        on = jnp.where(live > slot, 1.0, 0.0)
        full.append(on)
        half.append(jnp.where(neigh[slot : slot + 1, :] == home_id, 0.0, on))

    energy = jnp.zeros((8, clusters), f32)
    home_rows = [[None] * 8 for _ in range(3)]
    for p in range(8):
        home = [jnp.broadcast_to(tiles_ref[c * 8 + p : c * 8 + p + 1, :], (8, clusters)) for c in range(6)]
        upper = rank > p
        sums = [jnp.zeros((8, clusters), f32) for _ in range(3)]
        for slot in range(slots):
            cols = slice(slot * clusters, (slot + 1) * clusters)
            other = [gather_ref[c * 8 : (c + 1) * 8, cols] for c in range(6)]
            offset = [home[c] - other[c] for c in range(3)]
            dist_sq = offset[0] * offset[0] + offset[1] * offset[1] + offset[2] * offset[2]
            root = lax.rsqrt(1.0 + dist_sq)
            inverse = root * root
            repulse = home[3] * other[3] * inverse
            attract = home[4] * other[4]
            coulomb = home[5] * other[5] * root
            weight = jnp.where(upper, full[slot], half[slot])
            energy = energy + weight * (inverse * (repulse - attract) + coulomb)
            factor = weight * inverse * (inverse * (4.0 * repulse - 2.0 * attract) + coulomb)
            for c in range(3):
                term = factor * offset[c]
                sums[c] = sums[c] + term
                place = (slice(c * 8, (c + 1) * 8), cols)
                push_ref[place] = term if p == 0 else push_ref[place] + term
        for c in range(3):
            home_rows[c][p] = jnp.sum(sums[c], axis=0, keepdims=True)
    home_grad = jnp.concatenate([home_rows[c][p] for c in range(3) for p in range(8)], axis=0)
    back = jnp.concatenate(split_parts(push_ref[...], 2), axis=0)
    tile_grad = join_parts(dot_nt(back, select_ref[...]), 24, 2)
    own = to_atoms(tile_grad[:, :clusters] - home_grad, atoms)
    returned = to_atoms(tile_grad[:, clusters:], lanes)

    step_dots = jnp.zeros((memory, atoms), f32)
    diff_dots = jnp.zeros((memory, atoms), f32)
    moved = jnp.zeros((1, atoms), f32)
    for c in range(3):
        returned_ref[c : c + 1, :] = returned[c]
        displacement = coords_ref[c : c + 1, :] - anchor_ref[c : c + 1, :]
        moved = moved + displacement * displacement
        grad = own[c] + displacement
        grad_ref[c : c + 1, :] = grad
        wide = jnp.broadcast_to(grad, (memory, atoms))
        step_dots = step_dots + step_ref[c] * wide
        diff_dots = diff_dots + diff_ref[c] * wide
    step_sum = lane_sum(step_dots)
    diff_sum = lane_sum(diff_dots)
    energy_sum = lane_sum(jnp.sum(energy, axis=0, keepdims=True)) + 0.5 * lane_sum(moved)
    dots = placed_dots(step_sum, diff_sum)
    dots = dots + jnp.where(iota((1, 128), 1) == 2 * memory, energy_sum, 0.0)
    gram = jnp.sum(gram_ref[...], axis=0, keepdims=True)
    sub8 = iota((8, 128), 0)
    common_ref[...] = jnp.where(sub8 == 6, dots, jnp.where(sub8 == 7, gram, 0.0))


def placed_dots(step_sum, diff_sum):
    memory = step_sum.shape[0]
    sub = iota((memory, 128), 0)
    lane = iota((memory, 128), 1)
    dots = jnp.where(lane == sub, step_sum, 0.0) + jnp.where(lane == sub + memory, diff_sum, 0.0)
    return jnp.sum(dots, axis=0, keepdims=True)


def chunk_kernel(sizes, common_ref, returned_ref, fz_ref, fy_ref, fx_ref, px_ref, pe_ref, chunk_ref):
    face, edge, _ = sizes
    faces, _ = slab_order(sizes)
    rows = fy_ref.shape[0]
    memory = rows // 6
    returned = returned_ref[...]
    far_step = jnp.zeros((memory, face), f32)
    far_diff = jnp.zeros((memory, face), f32)
    for place, hist in enumerate((fz_ref[...], fy_ref[...], fx_ref[...])):
        for c in range(3):
            row = returned[c : c + 1, place * face : (place + 1) * face]
            wide = jnp.broadcast_to(row, (memory, face))
            far_step = far_step + hist[c * memory : (c + 1) * memory] * wide
            far_diff = far_diff + hist[(3 + c) * memory : (4 + c) * memory] * wide
    group = iota((1, 128), 1) // edge
    above_sum = jnp.zeros((memory, 128), f32)
    below_sum = jnp.zeros((memory, 128), f32)
    packs = (pe_ref[0:16, :], px_ref[16:32, :], px_ref[32:48, :], px_ref[48:64, :])
    tails = jnp.concatenate([returned[:, faces:], jnp.zeros((5, 128), f32)], axis=0)
    for place, pack in enumerate(packs):
        turned = [pltpu.roll(tails, (k - place) % 4 * edge, 1) for k in range(4)]
        above = jnp.where(
            group == 1, turned[1][1:2], jnp.where(group == 2, turned[2][0:1], jnp.where(group == 3, turned[3][2:3], 0.0))
        )
        below = jnp.where(
            group == 0, turned[0][0:1], jnp.where(group == 1, turned[1][2:3], jnp.where(group == 2, turned[2][1:2], 0.0))
        )
        above_sum = above_sum + pack[0:8] * jnp.broadcast_to(above, (memory, 128))
        below_sum = below_sum + pack[8:16] * jnp.broadcast_to(below, (memory, 128))
    both = above_sum + below_sum
    step_sum = lane_sum(far_step) + lane_sum(jnp.where(group < 2, both, 0.0))
    diff_sum = lane_sum(far_diff) + lane_sum(jnp.where(group < 2, 0.0, both))
    common = common_ref[...] + jnp.where(iota((8, 128), 0) == 6, placed_dots(step_sum, diff_sum), 0.0)
    for device in range(chunk_ref.shape[0]):
        chunk_ref[device] = common
    for code in range(1, 8):
        target = linear_device(code_bits(code))
        start = {1: 0, 2: face, 4: 2 * face}.get(code, faces)
        pieces = [returned[:, start : start + 128]]
        if code in (1, 2, 4):
            pieces.append(returned[:, start + 128 : start + 256])
        chunk_ref[target, 0 : 3 * len(pieces), :] = jnp.concatenate(pieces, axis=0)


def finish_kernel(sizes, atoms_total, recv_ref, send_ref, grad_ref, coords_ref, step_ref, diff_ref, new_ref, energy_ref):
    _, edge, _ = sizes
    faces, edges = slab_order(sizes)
    atoms = coords_ref.shape[1]
    memory = step_ref.shape[1]
    devices = recv_ref.shape[0]
    total = recv_ref[0]
    for device in range(1, devices):
        total = total + recv_ref[device]
    dots = jnp.broadcast_to(total[6:7, :], (memory, 128))
    gram = jnp.broadcast_to(total[7:8, :], (memory, 128))
    sub = iota((memory, 128), 0)
    lane = iota((memory, 128), 1)

    def pick(row, where):
        return jnp.broadcast_to(lane_sum(jnp.where(where, row, 0.0)), (memory, 128))

    def at(value, m):
        return jnp.broadcast_to(value[m : m + 1, :], (memory, 128))

    step_dots = pick(dots, lane == sub)
    diff_dots = pick(dots, lane == sub + memory)
    energy_ref[...] = lane_sum(jnp.where(iota((1, 128), 1) == 2 * memory, total[6:7, :], 0.0)) / atoms_total
    sy_col = [pick(gram, lane == sub * memory + j) for j in range(memory)]
    sy_row = [pick(gram, lane == j * memory + sub) for j in range(memory)]
    yy_col = [pick(gram, lane == memory * memory + sub * memory + j) for j in range(memory)]
    diagonal = pick(gram, lane == sub * (memory + 1))
    rho = 1.0 / diagonal
    last = memory - 1
    scaling = at(diagonal, last) / at(yy_col[last], last)
    left = step_dots
    alpha = jnp.zeros((memory, 128), f32)
    folded = diff_dots
    for m in reversed(range(memory)):
        value = at(left * rho, m)
        alpha = jnp.where(sub == m, value, alpha)
        left = left - value * sy_col[m]
        folded = folded - value * yy_col[m]
    left = diagonal * alpha - scaling * folded
    coef = jnp.zeros((memory, 128), f32)
    for m in range(memory):
        value = at(left * rho, m)
        coef = jnp.where(sub == m, value, coef)
        left = left - value * sy_row[m]
    diff_coef = -scaling * alpha

    blocks = {code: recv_ref[linear_device(tuple(-bit for bit in code_bits(code)))] for code in range(1, 8)}
    edge_lane = iota((8, 128), 1)
    tail = jnp.where(
        edge_lane < edge,
        blocks[3],
        jnp.where(edge_lane < 2 * edge, blocks[5], jnp.where(edge_lane < 3 * edge, blocks[6], blocks[7])),
    )
    tail = jnp.where(edge_lane < edges, tail, 0.0)
    pieces = []
    for code in (1, 2, 4):
        pieces += [blocks[code][0:3], blocks[code][3:6]]
    pieces.append(tail[0:3])
    returned = jnp.concatenate([jnp.concatenate(pieces, axis=1), jnp.zeros((5, faces + 128), f32)], axis=0)
    back = jnp.concatenate(split_parts(returned, 2), axis=0)
    send = send_ref[:, : faces + 128]
    added = []
    chunk = 256
    for first in range(0, atoms, chunk):
        added.append(join_parts(dot_nt(back, send_one_hot(send, first, chunk)), 8, 2))
    added = jnp.concatenate(added, axis=1)
    widen = atoms // 128
    for c in range(3):
        grad = grad_ref[c : c + 1, :] + added[c : c + 1, :]
        mixed = jnp.tile(coef, (1, widen)) * step_ref[c] + jnp.tile(diff_coef, (1, widen)) * diff_ref[c]
        direction = jnp.tile(scaling[0:1], (1, widen)) * grad + jnp.sum(mixed, axis=0, keepdims=True)
        new_ref[c : c + 1, :] = coords_ref[c : c + 1, :] - step_length * direction


def call(kernel, outs, scratch, *args, limit_mib=16, space=pltpu.VMEM):
    if space == pltpu.HBM:
        args = [pltpu.with_memory_space_constraint(arg, pltpu.HBM) for arg in args]
    return pl.pallas_call(
        kernel,
        out_shape=[jax.ShapeDtypeStruct(shape, dtype) for shape, dtype in outs],
        in_specs=[pl.BlockSpec(memory_space=space)] * len(args),
        out_specs=[pl.BlockSpec(memory_space=pltpu.VMEM)] * len(outs),
        scratch_shapes=scratch,
        compiler_params=pltpu.CompilerParams(vmem_limit_bytes=limit_mib << 20),
    )(*args)


def on_device(
    coords,
    anchor,
    atom_types,
    halo_send,
    neighbours,
    live_counts,
    rep_coef,
    disp_coef,
    charge,
    step_history,
    grad_history,
):
    atoms = coords.shape[1]
    clusters = atoms // 8
    memory = step_history.shape[0]
    sizes = export_sizes(atoms)
    face, edge, corner = sizes
    faces, _ = slab_order(sizes)
    lanes = faces + 128
    wide = pl.cdiv(lanes, 1024) * 1024
    slots = neighbours.shape[1]
    devices = lax.axis_size("gx") * lax.axis_size("gy") * lax.axis_size("gz")
    assert edge == 32 and corner <= edge and face == 256 and memory == 8
    steps = step_history.transpose(1, 0, 2)
    diffs = grad_history.transpose(1, 0, 2)
    neigh = neighbours.T
    live = live_counts[None]
    rows = 6 * memory

    ntypes = rep_coef.shape[0]
    pay_z, pay_y, pay_x, pay_e, far_z, far_y, far_x, params, order, coords_v, steps_v, diffs_v, anchor_v, neigh_v, live_v = call(
        functools.partial(export_kernel, sizes),
        [((32, 128), f32)] * 2
        + [((16, 128), f32), ((32, 128), f32)]
        + [((rows, face), f32)] * 3
        + [((8, atoms), f32), ((1, wide), i32)]
        + [(value.shape, value.dtype) for value in (coords, steps, diffs, anchor, neigh, live)],
        [
            pltpu.VMEM((8, atoms), f32),
            pltpu.VMEM((1, wide), i32),
            pltpu.VMEM(halo_send.shape, i32),
            pltpu.VMEM((1, atoms), i32),
            pltpu.VMEM((1, ntypes), f32),
            pltpu.VMEM((1, ntypes), f32),
            pltpu.VMEM((1, ntypes), f32),
            pltpu.SemaphoreType.DMA((11,)),
        ],
        halo_send, coords, atom_types[None], rep_coef[None], disp_coef[None], charge[None],
        steps, diffs, anchor, neigh, live,
        space=pltpu.HBM,
    )
    pe = shifted(pay_e, ("gy", "gz"), -1)
    py = shifted(pay_y, ("gy",), -1)
    pz = shifted(pay_z, ("gz",), -1)
    fx = shifted(far_x, ("gx",), -1)
    fy = shifted(far_y, ("gy",), -1)
    fz = shifted(far_z, ("gz",), -1)
    tiles, other = call(
        local_kernel,
        [((48, clusters), f32), ((48, slots * clusters), f32)],
        [],
        coords_v, params, neigh_v,
    )
    (pay_x,) = call(merge_kernel, [((64, 128), f32)], [], pay_x, pz, py, pe, limit_mib=4)
    px = shifted(pay_x, ("gx",), -1)
    (gram,) = call(gram_kernel, [((memory, 128), f32)], [], steps_v, diffs_v, limit_mib=8)
    grad, returned, common = call(
        functools.partial(pair_kernel, sizes),
        [((3, atoms), f32), ((3, lanes), f32), ((8, 128), f32)],
        [
            pltpu.VMEM((clusters + 128, slots * clusters), bf16),
            pltpu.VMEM((48, slots * clusters), f32),
            pltpu.VMEM((24, slots * clusters), f32),
        ],
        tiles, other, gram, pz, py, px, pe, neigh_v, live_v, coords_v, anchor_v, steps_v, diffs_v,
        limit_mib=24,
    )
    (chunks,) = call(
        functools.partial(chunk_kernel, sizes),
        [((devices, 8, 128), f32)],
        [],
        common, returned, fz, fy, fx, px, pe,
        limit_mib=24,
    )
    received = lax.all_to_all(chunks, AXES, 0, 0, tiled=True)
    new_coords, energy = call(
        functools.partial(finish_kernel, sizes, atoms * devices),
        [((3, atoms), f32), ((1, 1), f32)],
        [],
        received, order, grad, coords_v, steps_v, diffs_v,
    )
    return (new_coords, energy[0, 0])


def solution(mesh):
    placed = (
        P(None, AXES),
        P(None, AXES),
        P(AXES),
        P(AXES),
        P(AXES, None),
        P(AXES),
        P(),
        P(),
        P(),
        P(None, None, AXES),
        P(None, None, AXES),
    )

    return jax.shard_map(
        on_device,
        mesh=mesh,
        in_specs=placed,
        out_specs=(P(None, AXES), P()),
        check_vma=False,
    )
```

```python
import functools
import math

import jax
import jax.numpy as jnp
from jax import lax
from jax.experimental import pallas as pl
from jax.experimental.pallas import tpu as pltpu
from jax.sharding import PartitionSpec as P


domain_side = 3.0
step_length = 0.5
AXES = ("gx", "gy", "gz")
f32 = jnp.float32
bf16 = jnp.bfloat16
i32 = jnp.int32


def export_sizes(atoms_local):
    face_rows = atoms_local // 8
    edge_rows = max(atoms_local // 64, 8)
    corner_rows = max(atoms_local // 512, 8)
    return face_rows, edge_rows, corner_rows


def shifted(value, axes, steps):
    shape = [lax.axis_size(axis) for axis in axes]
    pairs = []
    for source in range(math.prod(shape)):
        rest, target, scale = source, 0, 1
        for count in reversed(shape):
            target += (rest % count + steps) % count * scale
            rest //= count
            scale *= count
        pairs.append((source, target))
    return lax.ppermute(value, axes, pairs)


def iota(shape, dim):
    return lax.broadcasted_iota(i32, shape, dim)


def split_parts(value, parts):
    pieces = []
    for part in range(parts):
        piece = value.astype(bf16)
        pieces.append(piece)
        if part + 1 < parts:
            value = value - piece.astype(f32)
    return pieces


def join_parts(stacked, rows, parts):
    total = stacked[(parts - 1) * rows :]
    for part in reversed(range(parts - 1)):
        total = total + stacked[part * rows : (part + 1) * rows]
    return total


def dot_nn(left, right):
    return lax.dot_general(left, right, (((1,), (0,)), ((), ())), preferred_element_type=f32)


def dot_nt(left, right):
    return lax.dot_general(left, right, (((1,), (1,)), ((), ())), preferred_element_type=f32)


def one_hot(condition):
    return jnp.where(condition, 1.0, 0.0).astype(bf16)


def slab_order(sizes):
    face, edge, corner = sizes
    return 3 * face, 3 * edge + corner


def reordered_send(send, sizes):
    face, edge, _ = sizes
    lane = iota(send.shape, 1)
    to_front = pltpu.roll(send, send.shape[1] - edge, 1)
    to_back = pltpu.roll(send, face, 1)
    moved = jnp.where(lane < 3 * face, to_front, to_back)
    return jnp.where((lane >= 2 * face) & (lane < 3 * face + edge), moved, send)


def chosen_rows(blocks, low, high, parts):
    rows = blocks[0].shape[0]
    stacked = jnp.concatenate(split_parts(jnp.concatenate(blocks, axis=0), parts), axis=0)
    found = join_parts(dot_nn(stacked, low), rows * len(blocks), parts)
    high = jnp.broadcast_to(high, (rows, high.shape[1]))
    total = None
    for block in range(len(blocks)):
        part = jnp.where(high == block, found[block * rows : (block + 1) * rows], 0.0)
        total = part if total is None else total + part
    return total


def type_table(rep_ref, disp_ref, charge_ref):
    sub = iota((8, rep_ref.shape[1]), 0)
    rows = jnp.where(sub == 1, disp_ref[...], jnp.where(sub == 2, charge_ref[...], 0.0))
    return jnp.where(sub == 0, rep_ref[...], rows)


def row_one_hot(values, first, rows):
    lanes = values.shape[1]
    near = jnp.clip(values - first, -1, rows).astype(f32).astype(bf16)
    column = iota((rows, 128), 0).astype(f32).astype(bf16)
    column = jnp.concatenate([column] * (lanes // 128), axis=1)
    return jnp.where(column == jnp.broadcast_to(near, (rows, lanes)), jnp.ones((), bf16), jnp.zeros((), bf16))


def export_kernel(
    sizes,
    send_hbm, coords_hbm, types_hbm, rep_hbm, disp_hbm, charge_hbm, step_hbm, diff_hbm, anchor_hbm, neigh_hbm, live_hbm,
    pay_z_ref, pay_y_ref, pay_x_ref, pay_e_ref,
    order_ref,
    coords_ref, step_ref, diff_ref, anchor_ref, neigh_ref, live_ref, types_ref, rep_ref, disp_ref, charge_ref,
    data_ref, send_pad_ref, send_ref, arrived,
):
    face, edge, _ = sizes
    faces, _ = slab_order(sizes)
    pairs = [
        (send_hbm, send_ref), (types_hbm, types_ref), (rep_hbm, rep_ref), (disp_hbm, disp_ref),
        (charge_hbm, charge_ref), (coords_hbm, coords_ref), (step_hbm, step_ref), (diff_hbm, diff_ref),
        (anchor_hbm, anchor_ref), (neigh_hbm, neigh_ref), (live_hbm, live_ref),
    ]
    copies = [pltpu.make_async_copy(source, place, arrived.at[k]) for k, (source, place) in enumerate(pairs)]
    for copy in copies:
        copy.start()
    for copy in copies[:6]:
        copy.wait()
    atoms = coords_ref.shape[1]
    ntypes = rep_ref.shape[1]
    send_pad_ref[...] = jnp.full(send_pad_ref.shape, -1, i32)
    count = send_ref.shape[0]
    for first in range(0, count, 128):
        width = min(128, count - first)
        send_pad_ref[:, first : first + width] = send_ref[pl.ds(first, width)].reshape(1, width)
    send = reordered_send(send_pad_ref[:, : faces + 128], sizes)
    order_ref[:, : faces + 128] = send
    high = send >> 7
    low = row_one_hot(send & 127, 0, 128)
    data_ref[0:3, :] = coords_ref[...]
    data_ref[3:4, :] = types_ref[...].astype(f32)
    data_ref[4:8, :] = jnp.zeros((4, atoms), f32)
    head = chosen_rows([data_ref[:, first : first + 128] for first in range(0, atoms, 128)], low, high, 3)
    kinds = row_one_hot(head[3:4].astype(i32), 0, ntypes)
    table = type_table(rep_ref, disp_ref, charge_ref)
    params = join_parts(dot_nn(jnp.concatenate(split_parts(table, 3), axis=0), kinds), 8, 3)
    head = jnp.where(iota(head.shape, 0) < 3, head, pltpu.roll(params, 3, 0))
    for copy in copies[6:]:
        copy.wait()
    hist = jnp.concatenate(
        [
            chosen_rows(
                [ref[c, :, first : first + 128] for first in range(0, atoms, 128)], low[:, faces:], high[:, faces:], 2
            )
            for ref in (step_ref, diff_ref)
            for c in range(3)
        ],
        axis=0,
    )
    tail = jnp.concatenate([head[:, faces:], hist, jnp.zeros((8, 128), f32)], axis=0)
    packs = [packed_slab(tail, place, edge) for place in range(4)]
    for place, (ref, pack) in enumerate(((pay_z_ref, 1), (pay_y_ref, 2), (pay_x_ref, None))):
        ref[0:8, :] = head[:, place * face : place * face + 128]
        ref[8:16, :] = head[:, place * face + 128 : (place + 1) * face]
        if pack is not None:
            ref[16:32, :] = packs[pack]
    pay_e_ref[0:16, :] = packs[0]
    pay_e_ref[16:32, :] = packs[3]


def history_kernel(step_ref, diff_ref, order_ref, far_z_ref, far_y_ref, far_x_ref):
    atoms = step_ref.shape[2]
    face = far_z_ref.shape[1]
    hist = jnp.concatenate([step_ref[...].reshape(-1, atoms), diff_ref[...].reshape(-1, atoms)], axis=0)
    left = jnp.concatenate(split_parts(hist, 2), axis=0)
    total = None
    chunk = 256
    for first in range(0, atoms, chunk):
        part = dot_nn(left[:, first : first + chunk], row_one_hot(order_ref[:, : 3 * face], first, chunk))
        total = part if total is None else total + part
    total = join_parts(total, hist.shape[0], 2)
    for place, ref in enumerate((far_z_ref, far_y_ref, far_x_ref)):
        ref[...] = total[:, place * face : (place + 1) * face]


def packed_slab(tail, place, edge):
    group = iota((16, 128), 1) // edge
    packed = jnp.zeros((16, 128), f32)
    for k in range(4):
        turned = pltpu.roll(tail[16 * k : 16 * k + 16], (k - place) % 4 * edge, 1)
        packed = jnp.where(group == k, turned, packed)
    return packed


def spread_rows(rows6, lanes):
    keep = (iota((8, lanes), 1) & 7) == iota((8, lanes), 0)
    return jnp.concatenate(
        [jnp.where(keep, jnp.broadcast_to(row, (8, lanes)), 0.0) for row in rows6], axis=0
    )


def to_clusters(rows6, cluster_row, clusters):
    lanes = rows6[0].shape[1]
    spread = spread_rows(rows6, lanes)
    left = jnp.concatenate(split_parts(spread, 3), axis=0)
    chosen = row_one_hot(cluster_row, 0, clusters)
    return join_parts(dot_nt(left, chosen), spread.shape[0], 3)


def to_atoms(tiles, lanes):
    rows = tiles.shape[0]
    blocks = lanes // 128
    group = iota((rows, 128), 1) >> 4
    picked = [
        jnp.where(group == block % 8, tiles[:, block // 8 * 128 : block // 8 * 128 + 128], 0.0) for block in range(blocks)
    ]
    spread = one_hot((iota((128, 128), 0) & 15) == (iota((128, 128), 1) >> 3))
    left = jnp.concatenate(split_parts(jnp.concatenate(picked, axis=0), 2), axis=0)
    wide = join_parts(dot_nn(left, spread), rows * blocks, 2)
    keep = (iota((8, 128), 1) & 7) == iota((8, 128), 0)
    result = []
    for comp in range(rows // 8):
        pieces = []
        for block in range(blocks):
            first = block * rows + comp * 8
            pieces.append(jnp.sum(jnp.where(keep, wide[first : first + 8], 0.0), axis=0, keepdims=True))
        result.append(jnp.concatenate(pieces, axis=1))
    return result


def lane_sum(value):
    return jnp.sum(value, axis=1, keepdims=True)


def local_kernel(
    coords_ref, types_ref, rep_ref, disp_ref, charge_ref, neigh_ref, tiles_ref, other_ref
):
    atoms = coords_ref.shape[1]
    clusters = atoms // 8
    slots = neigh_ref.shape[0]
    table = type_table(rep_ref, disp_ref, charge_ref)
    kinds = row_one_hot(types_ref[...], 0, table.shape[1])
    params = join_parts(dot_nn(jnp.concatenate(split_parts(table, 3), axis=0), kinds), 8, 3)
    rows6 = [coords_ref[c : c + 1, :] for c in range(3)] + [params[c : c + 1] for c in range(3)]
    tiles = to_clusters(rows6, iota((1, atoms), 1) >> 3, clusters)
    tiles_ref[...] = tiles
    left = jnp.concatenate(split_parts(tiles, 3), axis=0)
    rows = tiles.shape[0]
    for slot in range(slots):
        cols = slice(slot * clusters, (slot + 1) * clusters)
        select = row_one_hot(neigh_ref[slot : slot + 1, :], 0, clusters)
        other_ref[:, cols] = join_parts(dot_nn(left, select), rows, 3)


def gram_kernel(step_ref, diff_ref, gram_ref):
    memory, atoms = step_ref.shape[1:]
    lane = iota((memory, 128), 1)
    sub = iota((memory, 128), 0)
    placed = jnp.zeros((memory, 128), f32)
    for j in range(memory):
        sy = None
        yy = None
        for comp in range(3):
            row = jnp.broadcast_to(diff_ref[comp, j : j + 1, :], (memory, atoms))
            one = step_ref[comp] * row
            two = diff_ref[comp] * row
            sy = one if sy is None else sy + one
            yy = two if yy is None else yy + two
        placed = placed + jnp.where(lane == sub * memory + j, lane_sum(sy), 0.0)
        placed = placed + jnp.where(lane == memory * memory + sub * memory + j, lane_sum(yy), 0.0)
    gram_ref[...] = placed


def merge_kernel(pay_ref, pz_ref, py_ref, pe_ref, out_ref):
    out_ref[0:16, :] = pay_ref[...]
    out_ref[16:32, :] = pz_ref[16:32, :]
    out_ref[32:48, :] = py_ref[16:32, :]
    out_ref[48:64, :] = pe_ref[16:32, :]


def remapped(neigh, clusters, sizes):
    face, edge, _ = (size // 8 for size in sizes)
    edge_first = clusters + 2 * face
    shift = jnp.where(
        neigh >= edge_first + edge + face,
        0,
        jnp.where(neigh >= edge_first + edge, -edge, jnp.where(neigh >= edge_first, face, 0)),
    )
    return neigh + shift


def linear_device(offset):
    total = 0
    for axis, step in zip(AXES, offset):
        count = lax.axis_size(axis)
        total = total * count + (lax.axis_index(axis) + step + count) % count
    return total


def code_bits(code):
    return code // 4, code // 2 % 2, code % 2


def shifted_rows(rows, inside):
    moved = [rows[c : c + 1] + jnp.where(inside[c], domain_side, 0.0) for c in range(3)]
    return moved + [rows[c : c + 1] for c in range(3, 6)]


def prep_kernel(sizes, other_ref, neigh_ref, pz_ref, py_ref, pe_ref, near_ref, select_ref, low_ref):
    face, edge, _ = sizes
    slots, clusters = neigh_ref.shape
    faces, edges = slab_order(sizes)
    halves = [ref[first : first + 8, :] for ref in (pz_ref, py_ref) for first in (0, 8)]
    rows = jnp.concatenate(halves + [pe_ref[0:8, :]], axis=1)
    lanes = rows.shape[1]
    lane = iota((1, lanes), 1)
    inside = (lane < 0, lane >= face, (lane < face) | (lane >= 2 * face))
    used = lane < 2 * face + edge
    rows6 = [jnp.where(used, row, 0.0) for row in shifted_rows(rows, inside)]
    place = lane + jnp.where(lane < 2 * face, 0, face)
    tiles = to_clusters(rows6, place >> 3, select_ref.shape[0])
    left = jnp.concatenate(split_parts(tiles, 3), axis=0)
    neigh = remapped(neigh_ref[...], clusters, sizes) - clusters
    for slot in range(slots):
        cols = slice(slot * clusters, (slot + 1) * clusters)
        select = row_one_hot(neigh[slot : slot + 1, :], 0, select_ref.shape[0])
        select_ref[:, cols] = select
        low_ref[:, cols] = row_one_hot((neigh[slot : slot + 1, :] + clusters) & 127, 0, 128)
        near_ref[:, cols] = other_ref[:, cols] + join_parts(dot_nn(left, select), tiles.shape[0], 3)


def pair_kernel(
    sizes, tiles_ref, near_ref, low_ref, halo_select_ref, gram_ref, px_ref,
    neigh_ref, live_ref, coords_ref, anchor_ref, step_ref, diff_ref,
    grad_ref, returned_ref, common_ref,
    gather_ref, push_ref,
):
    face, edge, _ = sizes
    atoms = coords_ref.shape[1]
    clusters = atoms // 8
    slots = neigh_ref.shape[0]
    faces, edges = slab_order(sizes)
    lanes = faces + 128
    memory = step_ref.shape[1]

    group = iota((8, 128), 1) // edge
    tail = jnp.zeros((8, 128), f32)
    for place in (1, 2, 3):
        block = pltpu.roll(px_ref[16 * place : 16 * place + 8, :], place * edge, 1)
        tail = jnp.where(group == place, block, tail)
    rows = jnp.concatenate([px_ref[0:8, :], px_ref[8:16, :], tail], axis=1)
    lane = iota((1, face + 128), 1)
    inside = (lane >= 0, lane >= face + 2 * edge, ((lane >= face) & (lane < face + 2 * edge)) | (lane >= face + 3 * edge))
    used = (lane < face) | ((lane >= face + edge) & (lane < face + edges))
    rows6 = [jnp.where(used, row, 0.0) for row in shifted_rows(rows, inside)]
    tiles = to_clusters(rows6, (lane + 2 * face) >> 3, halo_select_ref.shape[0])
    left = jnp.concatenate(split_parts(tiles, 3), axis=0)
    for slot in range(slots):
        cols = slice(slot * clusters, (slot + 1) * clusters)
        far = dot_nn(left, halo_select_ref[:, cols])
        gather_ref[:, cols] = near_ref[:, cols] + join_parts(far, tiles.shape[0], 3)

    neigh = neigh_ref[...]
    rank = iota((8, clusters), 0)
    home_id = iota((8, clusters), 1)
    live = jnp.broadcast_to(live_ref[...], (8, clusters))
    full = []
    half = []
    for slot in range(slots):
        on = jnp.where(live > slot, 1.0, jnp.inf)
        full.append(on)
        half.append(jnp.where(neigh[slot : slot + 1, :] == home_id, jnp.inf, on))

    energy = jnp.zeros((8, clusters), f32)
    half_coulomb = jnp.zeros((8, clusters), f32)
    home_rows = [[None] * 8 for _ in range(3)]
    for p in range(8):
        home = [jnp.broadcast_to(tiles_ref[c * 8 + p : c * 8 + p + 1, :], (8, clusters)) for c in range(6)]
        home[5] = 0.5 * home[5]
        upper = rank > p
        sums = [jnp.zeros((8, clusters), f32) for _ in range(3)]
        for slot in range(slots):
            cols = slice(slot * clusters, (slot + 1) * clusters)
            other = [gather_ref[c * 8 : (c + 1) * 8, cols] for c in range(6)]
            offset = [home[c] - other[c] for c in range(3)]
            dist_sq = offset[0] * offset[0] + offset[1] * offset[1] + offset[2] * offset[2]
            root = lax.rsqrt(dist_sq + jnp.where(upper, full[slot], half[slot]))
            inverse = root * root
            repulse = home[3] * other[3] * inverse
            less = repulse - home[4] * other[4]
            coulomb = home[5] * other[5] * root
            energy = energy + inverse * less
            half_coulomb = half_coulomb + coulomb
            factor = inverse * (inverse * (repulse + less) + coulomb)
            for c in range(3):
                term = factor * offset[c]
                sums[c] = sums[c] + term
                place = (slice(c * 8, (c + 1) * 8), cols)
                push_ref[place] = term if p == 0 else push_ref[place] + term
        for c in range(3):
            home_rows[c][p] = jnp.sum(sums[c], axis=0, keepdims=True)
    energy = energy + 2.0 * half_coulomb
    home_grad = jnp.concatenate([home_rows[c][p] for c in range(3) for p in range(8)], axis=0)
    back = jnp.concatenate(split_parts(push_ref[...], 2), axis=0)
    high = remapped(neigh, clusters, sizes) >> 7
    high = jnp.concatenate([high[slot : slot + 1] for slot in range(slots)], axis=1).astype(f32).astype(bf16)
    high = jnp.broadcast_to(high, back.shape)
    held = clusters // 128 + 1
    masked = [jnp.where(high == jnp.array(block, bf16), back, jnp.zeros((), bf16)) for block in range(held)]
    tile_grad = dot_nt(jnp.concatenate(masked, axis=0), low_ref[...])
    tile_grad = [join_parts(tile_grad[48 * block : 48 * block + 48], 24, 2) for block in range(held)]
    own = to_atoms(2.0 * (jnp.concatenate(tile_grad[:-1], axis=1) - home_grad), atoms)
    returned = to_atoms(2.0 * tile_grad[-1], lanes)

    step_dots = jnp.zeros((memory, atoms), f32)
    diff_dots = jnp.zeros((memory, atoms), f32)
    moved = jnp.zeros((1, atoms), f32)
    for c in range(3):
        returned_ref[c : c + 1, :] = returned[c]
        displacement = coords_ref[c : c + 1, :] - anchor_ref[c : c + 1, :]
        moved = moved + displacement * displacement
        grad = own[c] + displacement
        grad_ref[c : c + 1, :] = grad
        wide = jnp.broadcast_to(grad, (memory, atoms))
        step_dots = step_dots + step_ref[c] * wide
        diff_dots = diff_dots + diff_ref[c] * wide
    step_sum = lane_sum(step_dots)
    diff_sum = lane_sum(diff_dots)
    energy_sum = lane_sum(jnp.sum(energy, axis=0, keepdims=True)) + 0.5 * lane_sum(moved)
    dots = placed_dots(step_sum, diff_sum)
    dots = dots + jnp.where(iota((1, 128), 1) == 2 * memory, energy_sum, 0.0)
    gram = jnp.sum(gram_ref[...], axis=0, keepdims=True)
    sub8 = iota((8, 128), 0)
    common_ref[...] = jnp.where(sub8 == 6, dots, jnp.where(sub8 == 7, gram, 0.0))


def placed_dots(step_sum, diff_sum):
    memory = step_sum.shape[0]
    sub = iota((memory, 128), 0)
    lane = iota((memory, 128), 1)
    dots = jnp.where(lane == sub, step_sum, 0.0) + jnp.where(lane == sub + memory, diff_sum, 0.0)
    return jnp.sum(dots, axis=0, keepdims=True)


def chunk_kernel(sizes, common_ref, returned_ref, fz_ref, fy_ref, fx_ref, px_ref, pe_ref, chunk_ref):
    face, edge, _ = sizes
    faces, _ = slab_order(sizes)
    rows = fy_ref.shape[0]
    memory = rows // 6
    returned = returned_ref[...]
    far_step = jnp.zeros((memory, face), f32)
    far_diff = jnp.zeros((memory, face), f32)
    for place, hist in enumerate((fz_ref[...], fy_ref[...], fx_ref[...])):
        for c in range(3):
            row = returned[c : c + 1, place * face : (place + 1) * face]
            wide = jnp.broadcast_to(row, (memory, face))
            far_step = far_step + hist[c * memory : (c + 1) * memory] * wide
            far_diff = far_diff + hist[(3 + c) * memory : (4 + c) * memory] * wide
    group = iota((1, 128), 1) // edge
    above_sum = jnp.zeros((memory, 128), f32)
    below_sum = jnp.zeros((memory, 128), f32)
    packs = (pe_ref[0:16, :], px_ref[16:32, :], px_ref[32:48, :], px_ref[48:64, :])
    tails = jnp.concatenate([returned[:, faces:], jnp.zeros((5, 128), f32)], axis=0)
    for place, pack in enumerate(packs):
        turned = [pltpu.roll(tails, (k - place) % 4 * edge, 1) for k in range(4)]
        above = jnp.where(
            group == 1, turned[1][1:2], jnp.where(group == 2, turned[2][0:1], jnp.where(group == 3, turned[3][2:3], 0.0))
        )
        below = jnp.where(
            group == 0, turned[0][0:1], jnp.where(group == 1, turned[1][2:3], jnp.where(group == 2, turned[2][1:2], 0.0))
        )
        above_sum = above_sum + pack[0:8] * jnp.broadcast_to(above, (memory, 128))
        below_sum = below_sum + pack[8:16] * jnp.broadcast_to(below, (memory, 128))
    both = above_sum + below_sum
    step_sum = lane_sum(far_step) + lane_sum(jnp.where(group < 2, both, 0.0))
    diff_sum = lane_sum(far_diff) + lane_sum(jnp.where(group < 2, 0.0, both))
    common = common_ref[...] + jnp.where(iota((8, 128), 0) == 6, placed_dots(step_sum, diff_sum), 0.0)
    for device in range(chunk_ref.shape[0]):
        chunk_ref[device] = common
    for code in range(1, 8):
        target = linear_device(code_bits(code))
        start = {1: 0, 2: face, 4: 2 * face}.get(code, faces)
        pieces = [returned[:, start : start + 128]]
        if code in (1, 2, 4):
            pieces.append(returned[:, start + 128 : start + 256])
        chunk_ref[target, 0 : 3 * len(pieces), :] = jnp.concatenate(pieces, axis=0)


def finish_kernel(sizes, atoms_total, recv_ref, order_ref, grad_ref, coords_ref, step_ref, diff_ref, new_ref, energy_ref):
    _, edge, _ = sizes
    faces, edges = slab_order(sizes)
    atoms = coords_ref.shape[1]
    memory = step_ref.shape[1]
    devices = recv_ref.shape[0]
    total = recv_ref[0]
    for device in range(1, devices):
        total = total + recv_ref[device]
    dots = jnp.broadcast_to(total[6:7, :], (memory, 128))
    gram = jnp.broadcast_to(total[7:8, :], (memory, 128))
    sub = iota((memory, 128), 0)
    lane = iota((memory, 128), 1)

    def pick(row, where):
        return jnp.broadcast_to(lane_sum(jnp.where(where, row, 0.0)), (memory, 128))

    def at(value, m):
        return jnp.broadcast_to(value[m : m + 1, :], (memory, 128))

    step_dots = pick(dots, lane == sub)
    diff_dots = pick(dots, lane == sub + memory)
    energy_ref[...] = lane_sum(jnp.where(iota((1, 128), 1) == 2 * memory, total[6:7, :], 0.0)) / atoms_total
    sy_col = [pick(gram, lane == sub * memory + j) for j in range(memory)]
    sy_row = [pick(gram, lane == j * memory + sub) for j in range(memory)]
    yy_col = [pick(gram, lane == memory * memory + sub * memory + j) for j in range(memory)]
    diagonal = pick(gram, lane == sub * (memory + 1))
    rho = 1.0 / diagonal
    last = memory - 1
    scaling = at(diagonal, last) / at(yy_col[last], last)
    left = step_dots
    alpha = jnp.zeros((memory, 128), f32)
    folded = diff_dots
    for m in reversed(range(memory)):
        value = at(left * rho, m)
        alpha = jnp.where(sub == m, value, alpha)
        left = left - value * sy_col[m]
        folded = folded - value * yy_col[m]
    left = diagonal * alpha - scaling * folded
    coef = jnp.zeros((memory, 128), f32)
    for m in range(memory):
        value = at(left * rho, m)
        coef = jnp.where(sub == m, value, coef)
        left = left - value * sy_row[m]
    diff_coef = -scaling * alpha

    blocks = {code: recv_ref[linear_device(tuple(-bit for bit in code_bits(code)))] for code in range(1, 8)}
    edge_lane = iota((8, 128), 1)
    tail = jnp.where(
        edge_lane < edge,
        blocks[3],
        jnp.where(edge_lane < 2 * edge, blocks[5], jnp.where(edge_lane < 3 * edge, blocks[6], blocks[7])),
    )
    tail = jnp.where(edge_lane < edges, tail, 0.0)
    pieces = []
    for code in (1, 2, 4):
        pieces += [blocks[code][0:3], blocks[code][3:6]]
    pieces.append(tail[0:3])
    returned = jnp.concatenate(pieces, axis=1)
    send = order_ref[:, : faces + 128]
    blocks = atoms // 128
    high = jnp.broadcast_to(send >> 7, (blocks, faces + 128)) == iota((blocks, faces + 128), 0)
    spread = [jnp.where(high, jnp.broadcast_to(returned[c : c + 1], high.shape), 0.0) for c in range(3)]
    back = jnp.concatenate(split_parts(jnp.concatenate(spread, axis=0), 2), axis=0)
    tiles = join_parts(dot_nt(back, row_one_hot(send & 127, 0, 128)), 3 * blocks, 2)
    added = [
        jnp.concatenate([tiles[c * blocks + block : c * blocks + block + 1] for block in range(blocks)], axis=1)
        for c in range(3)
    ]
    widen = atoms // 128
    for c in range(3):
        grad = grad_ref[c : c + 1, :] + added[c]
        mixed = jnp.tile(coef, (1, widen)) * step_ref[c] + jnp.tile(diff_coef, (1, widen)) * diff_ref[c]
        direction = jnp.tile(scaling[0:1], (1, widen)) * grad + jnp.sum(mixed, axis=0, keepdims=True)
        new_ref[c : c + 1, :] = coords_ref[c : c + 1, :] - step_length * direction


def call(kernel, outs, scratch, *args, limit_mib=16, space=pltpu.VMEM):
    if space == pltpu.HBM:
        args = [pltpu.with_memory_space_constraint(arg, pltpu.HBM) for arg in args]
    return pl.pallas_call(
        kernel,
        out_shape=[jax.ShapeDtypeStruct(shape, dtype) for shape, dtype in outs],
        in_specs=[pl.BlockSpec(memory_space=space)] * len(args),
        out_specs=[pl.BlockSpec(memory_space=pltpu.VMEM)] * len(outs),
        scratch_shapes=scratch,
        compiler_params=pltpu.CompilerParams(vmem_limit_bytes=limit_mib << 20),
    )(*args)


def on_device(
    coords,
    anchor,
    atom_types,
    halo_send,
    neighbours,
    live_counts,
    rep_coef,
    disp_coef,
    charge,
    step_history,
    grad_history,
):
    atoms = coords.shape[1]
    clusters = atoms // 8
    memory = step_history.shape[0]
    sizes = export_sizes(atoms)
    face, edge, corner = sizes
    faces, _ = slab_order(sizes)
    lanes = faces + 128
    wide = pl.cdiv(lanes, 1024) * 1024
    slots = neighbours.shape[1]
    devices = lax.axis_size("gx") * lax.axis_size("gy") * lax.axis_size("gz")
    assert edge == 32 and corner <= edge and face == 256 and memory == 8
    steps = step_history.transpose(1, 0, 2)
    diffs = grad_history.transpose(1, 0, 2)
    neigh = neighbours.T
    live = live_counts[None]
    rows = 6 * memory

    types, tables = atom_types[None], [table[None] for table in (rep_coef, disp_coef, charge)]
    pay_z, pay_y, pay_x, pay_e, order, coords_v, steps_v, diffs_v, anchor_v, neigh_v, live_v, *types_v = call(
        functools.partial(export_kernel, sizes),
        [((32, 128), f32)] * 2
        + [((16, 128), f32), ((32, 128), f32), ((1, wide), i32)]
        + [(value.shape, value.dtype) for value in (coords, steps, diffs, anchor, neigh, live, types, *tables)],
        [
            pltpu.VMEM((8, atoms), f32),
            pltpu.VMEM((1, wide), i32),
            pltpu.VMEM(halo_send.shape, i32),
            pltpu.SemaphoreType.DMA((11,)),
        ],
        halo_send, coords, types, *tables,
        steps, diffs, anchor, neigh, live,
        space=pltpu.HBM,
    )
    pe = shifted(pay_e, ("gy", "gz"), -1)
    py = shifted(pay_y, ("gy",), -1)
    pz = shifted(pay_z, ("gz",), -1)
    far_z, far_y, far_x = call(history_kernel, [((rows, face), f32)] * 3, [], steps_v, diffs_v, order)
    fx = shifted(far_x, ("gx",), -1)
    fy = shifted(far_y, ("gy",), -1)
    fz = shifted(far_z, ("gz",), -1)
    tiles, other = call(
        local_kernel,
        [((48, clusters), f32), ((48, slots * clusters), f32)],
        [],
        coords_v, *types_v, neigh_v,
    )
    (pay_x,) = call(merge_kernel, [((64, 128), f32)], [], pay_x, pz, py, pe, limit_mib=4)
    px = shifted(pay_x, ("gx",), -1)
    near, halo_select, low_select = call(
        functools.partial(prep_kernel, sizes),
        [((48, slots * clusters), f32)] + [((128, slots * clusters), bf16)] * 2,
        [],
        other, neigh_v, pz, py, pe,
    )
    (gram,) = call(gram_kernel, [((memory, 128), f32)], [], steps_v, diffs_v, limit_mib=8)
    grad, returned, common = call(
        functools.partial(pair_kernel, sizes),
        [((3, atoms), f32), ((3, lanes), f32), ((8, 128), f32)],
        [pltpu.VMEM((48, slots * clusters), f32), pltpu.VMEM((24, slots * clusters), f32)],
        tiles, near, low_select, halo_select, gram, px, neigh_v, live_v, coords_v, anchor_v, steps_v, diffs_v,
        limit_mib=16,
    )
    (chunks,) = call(
        functools.partial(chunk_kernel, sizes),
        [((devices, 8, 128), f32)],
        [],
        common, returned, fz, fy, fx, px, pe,
        limit_mib=24,
    )
    received = lax.all_to_all(chunks, AXES, 0, 0, tiled=True)
    new_coords, energy = call(
        functools.partial(finish_kernel, sizes, atoms * devices),
        [((3, atoms), f32), ((1, 1), f32)],
        [],
        received, order, grad, coords_v, steps_v, diffs_v,
    )
    return (new_coords, energy[0, 0])


def solution(mesh):
    placed = (
        P(None, AXES),
        P(None, AXES),
        P(AXES),
        P(AXES),
        P(AXES, None),
        P(AXES),
        P(),
        P(),
        P(),
        P(None, None, AXES),
        P(None, None, AXES),
    )

    return jax.shard_map(
        on_device,
        mesh=mesh,
        in_specs=placed,
        out_specs=(P(None, AXES), P()),
        check_vma=False,
    )
```

```python
import functools
import math

import jax
import jax.numpy as jnp
from jax import lax
from jax.experimental import pallas as pl
from jax.experimental.pallas import tpu as pltpu
from jax.sharding import PartitionSpec as P


domain_side = 3.0
step_length = 0.5
AXES = ("gx", "gy", "gz")
f32 = jnp.float32
bf16 = jnp.bfloat16
i32 = jnp.int32


def export_sizes(atoms_local):
    face_rows = atoms_local // 8
    edge_rows = max(atoms_local // 64, 8)
    corner_rows = max(atoms_local // 512, 8)
    return face_rows, edge_rows, corner_rows


def shifted(value, axes, steps):
    shape = [lax.axis_size(axis) for axis in axes]
    pairs = []
    for source in range(math.prod(shape)):
        rest, target, scale = source, 0, 1
        for count in reversed(shape):
            target += (rest % count + steps) % count * scale
            rest //= count
            scale *= count
        pairs.append((source, target))
    return lax.ppermute(value, axes, pairs)


def iota(shape, dim):
    return lax.broadcasted_iota(i32, shape, dim)


def split_parts(value, parts):
    pieces = []
    for part in range(parts):
        piece = value.astype(bf16)
        pieces.append(piece)
        if part + 1 < parts:
            value = value - piece.astype(f32)
    return pieces


def join_parts(stacked, rows, parts):
    total = stacked[(parts - 1) * rows :]
    for part in reversed(range(parts - 1)):
        total = total + stacked[part * rows : (part + 1) * rows]
    return total


def dot_nn(left, right):
    return lax.dot_general(left, right, (((1,), (0,)), ((), ())), preferred_element_type=f32)


def dot_nt(left, right):
    return lax.dot_general(left, right, (((1,), (1,)), ((), ())), preferred_element_type=f32)


def one_hot(condition):
    return jnp.where(condition, 1.0, 0.0).astype(bf16)


def slab_order(sizes):
    face, edge, corner = sizes
    return 3 * face, 3 * edge + corner


def reordered_send(send, sizes):
    face, edge, _ = sizes
    lane = iota(send.shape, 1)
    to_front = pltpu.roll(send, send.shape[1] - edge, 1)
    to_back = pltpu.roll(send, face, 1)
    moved = jnp.where(lane < 3 * face, to_front, to_back)
    return jnp.where((lane >= 2 * face) & (lane < 3 * face + edge), moved, send)


def chosen_rows(blocks, low, high, parts):
    rows = blocks[0].shape[0]
    stacked = jnp.concatenate(split_parts(jnp.concatenate(blocks, axis=0), parts), axis=0)
    found = join_parts(dot_nn(stacked, low), rows * len(blocks), parts)
    high = jnp.broadcast_to(high, (rows, high.shape[1]))
    total = None
    for block in range(len(blocks)):
        part = jnp.where(high == block, found[block * rows : (block + 1) * rows], 0.0)
        total = part if total is None else total + part
    return total


def type_table(rep_ref, disp_ref, charge_ref):
    sub = iota((8, rep_ref.shape[1]), 0)
    rows = jnp.where(sub == 1, disp_ref[...], jnp.where(sub == 2, charge_ref[...], 0.0))
    return jnp.where(sub == 0, rep_ref[...], rows)


def row_one_hot(values, first, rows):
    lanes = values.shape[1]
    near = jnp.clip(values - first, -1, rows).astype(f32).astype(bf16)
    column = iota((rows, 128), 0).astype(f32).astype(bf16)
    column = jnp.concatenate([column] * (lanes // 128), axis=1)
    return jnp.where(column == jnp.broadcast_to(near, (rows, lanes)), jnp.ones((), bf16), jnp.zeros((), bf16))


def export_kernel(
    sizes,
    send_hbm, coords_hbm, types_hbm, rep_hbm, disp_hbm, charge_hbm, step_hbm, diff_hbm, anchor_hbm, neigh_hbm, live_hbm,
    pay_z_ref, pay_y_ref, pay_x_ref, pay_e_ref,
    order_ref,
    coords_ref, step_ref, diff_ref, anchor_ref, neigh_ref, live_ref, types_ref, rep_ref, disp_ref, charge_ref,
    data_ref, send_pad_ref, send_ref, arrived,
):
    face, edge, _ = sizes
    faces, _ = slab_order(sizes)
    pairs = [
        (send_hbm, send_ref), (types_hbm, types_ref), (rep_hbm, rep_ref), (disp_hbm, disp_ref),
        (charge_hbm, charge_ref), (coords_hbm, coords_ref), (step_hbm, step_ref), (diff_hbm, diff_ref),
        (anchor_hbm, anchor_ref), (neigh_hbm, neigh_ref), (live_hbm, live_ref),
    ]
    copies = [pltpu.make_async_copy(source, place, arrived.at[k]) for k, (source, place) in enumerate(pairs)]
    for copy in copies:
        copy.start()
    for copy in copies[:6]:
        copy.wait()
    atoms = coords_ref.shape[1]
    ntypes = rep_ref.shape[1]
    send_pad_ref[...] = jnp.full(send_pad_ref.shape, -1, i32)
    count = send_ref.shape[0]
    for first in range(0, count, 128):
        width = min(128, count - first)
        send_pad_ref[:, first : first + width] = send_ref[pl.ds(first, width)].reshape(1, width)
    send = reordered_send(send_pad_ref[:, : faces + 128], sizes)
    order_ref[:, : faces + 128] = send
    high = send >> 7
    low = row_one_hot(send & 127, 0, 128)
    data_ref[0:3, :] = coords_ref[...]
    data_ref[3:4, :] = types_ref[...].astype(f32)
    data_ref[4:8, :] = jnp.zeros((4, atoms), f32)
    head = chosen_rows([data_ref[:, first : first + 128] for first in range(0, atoms, 128)], low, high, 3)
    kinds = row_one_hot(head[3:4].astype(i32), 0, ntypes)
    table = type_table(rep_ref, disp_ref, charge_ref)
    params = join_parts(dot_nn(jnp.concatenate(split_parts(table, 3), axis=0), kinds), 8, 3)
    head = jnp.where(iota(head.shape, 0) < 3, head, pltpu.roll(params, 3, 0))
    for copy in copies[6:]:
        copy.wait()
    hist = jnp.concatenate(
        [
            chosen_rows(
                [ref[c, :, first : first + 128] for first in range(0, atoms, 128)], low[:, faces:], high[:, faces:], 2
            )
            for ref in (step_ref, diff_ref)
            for c in range(3)
        ],
        axis=0,
    )
    tail = jnp.concatenate([head[:, faces:], hist, jnp.zeros((8, 128), f32)], axis=0)
    packs = [packed_slab(tail, place, edge) for place in range(4)]
    for place, (ref, pack) in enumerate(((pay_z_ref, 1), (pay_y_ref, 2), (pay_x_ref, None))):
        ref[0:8, :] = head[:, place * face : place * face + 128]
        ref[8:16, :] = head[:, place * face + 128 : (place + 1) * face]
        if pack is not None:
            ref[16:32, :] = packs[pack]
    pay_e_ref[0:16, :] = packs[0]
    pay_e_ref[16:32, :] = packs[3]


def history_kernel(step_ref, diff_ref, order_ref, far_z_ref, far_y_ref, far_x_ref):
    atoms = step_ref.shape[2]
    face = far_z_ref.shape[1]
    hist = jnp.concatenate([step_ref[...].reshape(-1, atoms), diff_ref[...].reshape(-1, atoms)], axis=0)
    left = jnp.concatenate(split_parts(hist, 2), axis=0)
    total = None
    chunk = 256
    for first in range(0, atoms, chunk):
        part = dot_nn(left[:, first : first + chunk], row_one_hot(order_ref[:, : 3 * face], first, chunk))
        total = part if total is None else total + part
    total = join_parts(total, hist.shape[0], 2)
    for place, ref in enumerate((far_z_ref, far_y_ref, far_x_ref)):
        ref[...] = total[:, place * face : (place + 1) * face]


def packed_slab(tail, place, edge):
    group = iota((16, 128), 1) // edge
    packed = jnp.zeros((16, 128), f32)
    for k in range(4):
        turned = pltpu.roll(tail[16 * k : 16 * k + 16], (k - place) % 4 * edge, 1)
        packed = jnp.where(group == k, turned, packed)
    return packed


def spread_rows(rows6, lanes):
    keep = (iota((8, lanes), 1) & 7) == iota((8, lanes), 0)
    return jnp.concatenate(
        [jnp.where(keep, jnp.broadcast_to(row, (8, lanes)), 0.0) for row in rows6], axis=0
    )


def to_clusters(rows6, cluster_row, clusters):
    lanes = rows6[0].shape[1]
    spread = spread_rows(rows6, lanes)
    left = jnp.concatenate(split_parts(spread, 3), axis=0)
    chosen = row_one_hot(cluster_row, 0, clusters)
    return join_parts(dot_nt(left, chosen), spread.shape[0], 3)


def to_atoms(tiles, lanes):
    rows = tiles.shape[0]
    blocks = lanes // 128
    group = iota((rows, 128), 1) >> 4
    picked = [
        jnp.where(group == block % 8, tiles[:, block // 8 * 128 : block // 8 * 128 + 128], 0.0) for block in range(blocks)
    ]
    spread = one_hot((iota((128, 128), 0) & 15) == (iota((128, 128), 1) >> 3))
    left = jnp.concatenate(split_parts(jnp.concatenate(picked, axis=0), 2), axis=0)
    wide = join_parts(dot_nn(left, spread), rows * blocks, 2)
    keep = (iota((8, 128), 1) & 7) == iota((8, 128), 0)
    result = []
    for comp in range(rows // 8):
        pieces = []
        for block in range(blocks):
            first = block * rows + comp * 8
            pieces.append(jnp.sum(jnp.where(keep, wide[first : first + 8], 0.0), axis=0, keepdims=True))
        result.append(jnp.concatenate(pieces, axis=1))
    return result


def lane_sum(value):
    return jnp.sum(value, axis=1, keepdims=True)


def local_kernel(
    coords_ref, types_ref, rep_ref, disp_ref, charge_ref, neigh_ref, tiles_ref, other_ref
):
    atoms = coords_ref.shape[1]
    clusters = atoms // 8
    slots = neigh_ref.shape[0]
    table = type_table(rep_ref, disp_ref, charge_ref)
    kinds = row_one_hot(types_ref[...], 0, table.shape[1])
    params = join_parts(dot_nn(jnp.concatenate(split_parts(table, 3), axis=0), kinds), 8, 3)
    rows6 = [coords_ref[c : c + 1, :] for c in range(3)] + [params[c : c + 1] for c in range(3)]
    tiles = to_clusters(rows6, iota((1, atoms), 1) >> 3, clusters)
    tiles_ref[...] = tiles
    left = jnp.concatenate(split_parts(tiles, 3), axis=0)
    rows = tiles.shape[0]
    for slot in range(slots):
        cols = slice(slot * clusters, (slot + 1) * clusters)
        select = row_one_hot(neigh_ref[slot : slot + 1, :], 0, clusters)
        other_ref[:, cols] = join_parts(dot_nn(left, select), rows, 3)


def gram_kernel(step_ref, diff_ref, gram_ref):
    memory, atoms = step_ref.shape[1:]
    lane = iota((memory, 128), 1)
    sub = iota((memory, 128), 0)
    placed = jnp.zeros((memory, 128), f32)
    for j in range(memory):
        sy = None
        yy = None
        for comp in range(3):
            row = jnp.broadcast_to(diff_ref[comp, j : j + 1, :], (memory, atoms))
            one = step_ref[comp] * row
            two = diff_ref[comp] * row
            sy = one if sy is None else sy + one
            yy = two if yy is None else yy + two
        placed = placed + jnp.where(lane == sub * memory + j, lane_sum(sy), 0.0)
        placed = placed + jnp.where(lane == memory * memory + sub * memory + j, lane_sum(yy), 0.0)
    gram_ref[...] = placed


def merge_kernel(edge, pay_ref, pz_ref, py_ref, pe_ref, out_ref, rest_ref):
    out_ref[0:16, :] = pay_ref[...]
    group = iota((8, 128), 1) // edge
    tail = jnp.zeros((8, 128), f32)
    for place, ref in ((1, pz_ref), (2, py_ref), (3, pe_ref)):
        tail = jnp.where(group == place, pltpu.roll(ref[16:24, :], place * edge, 1), tail)
        rest_ref[16 * place - 16 : 16 * place, :] = ref[16:32, :]
    out_ref[16:24, :] = tail


def remapped(neigh, clusters, sizes):
    face, edge, _ = (size // 8 for size in sizes)
    edge_first = clusters + 2 * face
    shift = jnp.where(
        neigh >= edge_first + edge + face,
        0,
        jnp.where(neigh >= edge_first + edge, -edge, jnp.where(neigh >= edge_first, face, 0)),
    )
    return neigh + shift


def linear_device(offset):
    total = 0
    for axis, step in zip(AXES, offset):
        count = lax.axis_size(axis)
        total = total * count + (lax.axis_index(axis) + step + count) % count
    return total


def code_bits(code):
    return code // 4, code // 2 % 2, code % 2


def shifted_rows(rows, inside):
    moved = [rows[c : c + 1] + jnp.where(inside[c], domain_side, 0.0) for c in range(3)]
    return moved + [rows[c : c + 1] for c in range(3, 6)]


def prep_kernel(sizes, other_ref, neigh_ref, pz_ref, py_ref, pe_ref, near_ref, select_ref, low_ref):
    face, edge, _ = sizes
    slots, clusters = neigh_ref.shape
    faces, edges = slab_order(sizes)
    halves = [ref[first : first + 8, :] for ref in (pz_ref, py_ref) for first in (0, 8)]
    rows = jnp.concatenate(halves + [pe_ref[0:8, :]], axis=1)
    lanes = rows.shape[1]
    lane = iota((1, lanes), 1)
    inside = (lane < 0, lane >= face, (lane < face) | (lane >= 2 * face))
    used = lane < 2 * face + edge
    rows6 = [jnp.where(used, row, 0.0) for row in shifted_rows(rows, inside)]
    place = lane + jnp.where(lane < 2 * face, 0, face)
    tiles = to_clusters(rows6, place >> 3, select_ref.shape[0])
    left = jnp.concatenate(split_parts(tiles, 3), axis=0)
    neigh = remapped(neigh_ref[...], clusters, sizes) - clusters
    for slot in range(slots):
        cols = slice(slot * clusters, (slot + 1) * clusters)
        select = row_one_hot(neigh[slot : slot + 1, :], 0, select_ref.shape[0])
        select_ref[:, cols] = select
        low_ref[:, cols] = row_one_hot((neigh[slot : slot + 1, :] + clusters) & 127, 0, 128)
        near_ref[:, cols] = other_ref[:, cols] + join_parts(dot_nn(left, select), tiles.shape[0], 3)


def pair_kernel(
    sizes, tiles_ref, near_ref, low_ref, halo_select_ref, gram_ref, px_ref,
    neigh_ref, live_ref, coords_ref, anchor_ref, step_ref, diff_ref,
    grad_ref, returned_ref, common_ref,
    gather_ref, push_ref,
):
    face, edge, _ = sizes
    atoms = coords_ref.shape[1]
    clusters = atoms // 8
    slots = neigh_ref.shape[0]
    faces, edges = slab_order(sizes)
    lanes = faces + 128
    memory = step_ref.shape[1]

    rows = jnp.concatenate([px_ref[first : first + 8, :] for first in (0, 8, 16)], axis=1)
    lane = iota((1, face + 128), 1)
    inside = (lane >= 0, lane >= face + 2 * edge, ((lane >= face) & (lane < face + 2 * edge)) | (lane >= face + 3 * edge))
    used = (lane < face) | ((lane >= face + edge) & (lane < face + edges))
    rows6 = [jnp.where(used, row, 0.0) for row in shifted_rows(rows, inside)]
    tiles = to_clusters(rows6, (lane + 2 * face) >> 3, halo_select_ref.shape[0])
    left = jnp.concatenate(split_parts(tiles, 3), axis=0)
    for slot in range(slots):
        cols = slice(slot * clusters, (slot + 1) * clusters)
        far = dot_nn(left, halo_select_ref[:, cols])
        gather_ref[:, cols] = near_ref[:, cols] + join_parts(far, tiles.shape[0], 3)

    neigh = neigh_ref[...]
    rank = iota((8, clusters), 0)
    home_id = iota((8, clusters), 1)
    live = jnp.broadcast_to(live_ref[...], (8, clusters))
    full = []
    half = []
    for slot in range(slots):
        on = jnp.where(live > slot, 1.0, jnp.inf)
        full.append(on)
        half.append(jnp.where(neigh[slot : slot + 1, :] == home_id, jnp.inf, on))

    energy = jnp.zeros((8, clusters), f32)
    half_coulomb = jnp.zeros((8, clusters), f32)
    home_rows = [[None] * 8 for _ in range(3)]
    for p in range(8):
        home = [jnp.broadcast_to(tiles_ref[c * 8 + p : c * 8 + p + 1, :], (8, clusters)) for c in range(6)]
        home[5] = 0.5 * home[5]
        upper = rank > p
        sums = [jnp.zeros((8, clusters), f32) for _ in range(3)]
        for slot in range(slots):
            cols = slice(slot * clusters, (slot + 1) * clusters)
            other = [gather_ref[c * 8 : (c + 1) * 8, cols] for c in range(6)]
            offset = [home[c] - other[c] for c in range(3)]
            dist_sq = offset[0] * offset[0] + offset[1] * offset[1] + offset[2] * offset[2]
            root = lax.rsqrt(dist_sq + jnp.where(upper, full[slot], half[slot]))
            inverse = root * root
            repulse = home[3] * other[3] * inverse
            less = repulse - home[4] * other[4]
            coulomb = home[5] * other[5] * root
            energy = energy + inverse * less
            half_coulomb = half_coulomb + coulomb
            factor = inverse * (inverse * (repulse + less) + coulomb)
            for c in range(3):
                term = factor * offset[c]
                sums[c] = sums[c] + term
                place = (slice(c * 8, (c + 1) * 8), cols)
                push_ref[place] = term if p == 0 else push_ref[place] + term
        for c in range(3):
            home_rows[c][p] = jnp.sum(sums[c], axis=0, keepdims=True)
    energy = energy + 2.0 * half_coulomb
    home_grad = jnp.concatenate([home_rows[c][p] for c in range(3) for p in range(8)], axis=0)
    back = jnp.concatenate(split_parts(push_ref[...], 2), axis=0)
    high = remapped(neigh, clusters, sizes) >> 7
    high = jnp.concatenate([high[slot : slot + 1] for slot in range(slots)], axis=1).astype(f32).astype(bf16)
    high = jnp.broadcast_to(high, back.shape)
    held = clusters // 128 + 1
    masked = [jnp.where(high == jnp.array(block, bf16), back, jnp.zeros((), bf16)) for block in range(held)]
    tile_grad = dot_nt(jnp.concatenate(masked, axis=0), low_ref[...])
    tile_grad = [join_parts(tile_grad[48 * block : 48 * block + 48], 24, 2) for block in range(held)]
    own = to_atoms(2.0 * (jnp.concatenate(tile_grad[:-1], axis=1) - home_grad), atoms)
    returned = to_atoms(2.0 * tile_grad[-1], lanes)

    step_dots = jnp.zeros((memory, atoms), f32)
    diff_dots = jnp.zeros((memory, atoms), f32)
    moved = jnp.zeros((1, atoms), f32)
    for c in range(3):
        returned_ref[c : c + 1, :] = returned[c]
        displacement = coords_ref[c : c + 1, :] - anchor_ref[c : c + 1, :]
        moved = moved + displacement * displacement
        grad = own[c] + displacement
        grad_ref[c : c + 1, :] = grad
        wide = jnp.broadcast_to(grad, (memory, atoms))
        step_dots = step_dots + step_ref[c] * wide
        diff_dots = diff_dots + diff_ref[c] * wide
    step_sum = lane_sum(step_dots)
    diff_sum = lane_sum(diff_dots)
    energy_sum = lane_sum(jnp.sum(energy, axis=0, keepdims=True)) + 0.5 * lane_sum(moved)
    dots = placed_dots(step_sum, diff_sum)
    dots = dots + jnp.where(iota((1, 128), 1) == 2 * memory, energy_sum, 0.0)
    gram = jnp.sum(gram_ref[...], axis=0, keepdims=True)
    sub8 = iota((8, 128), 0)
    common_ref[...] = jnp.where(sub8 == 6, dots, jnp.where(sub8 == 7, gram, 0.0))


def placed_dots(step_sum, diff_sum):
    memory = step_sum.shape[0]
    sub = iota((memory, 128), 0)
    lane = iota((memory, 128), 1)
    dots = jnp.where(lane == sub, step_sum, 0.0) + jnp.where(lane == sub + memory, diff_sum, 0.0)
    return jnp.sum(dots, axis=0, keepdims=True)


def chunk_kernel(sizes, common_ref, returned_ref, fz_ref, fy_ref, fx_ref, fe_ref, pe_ref, chunk_ref):
    face, edge, _ = sizes
    faces, _ = slab_order(sizes)
    rows = fy_ref.shape[0]
    memory = rows // 6
    returned = returned_ref[...]
    far_step = jnp.zeros((memory, face), f32)
    far_diff = jnp.zeros((memory, face), f32)
    for place, hist in enumerate((fz_ref[...], fy_ref[...], fx_ref[...])):
        for c in range(3):
            row = returned[c : c + 1, place * face : (place + 1) * face]
            wide = jnp.broadcast_to(row, (memory, face))
            far_step = far_step + hist[c * memory : (c + 1) * memory] * wide
            far_diff = far_diff + hist[(3 + c) * memory : (4 + c) * memory] * wide
    group = iota((1, 128), 1) // edge
    above_sum = jnp.zeros((memory, 128), f32)
    below_sum = jnp.zeros((memory, 128), f32)
    packs = (pe_ref[0:16, :], fe_ref[0:16, :], fe_ref[16:32, :], fe_ref[32:48, :])
    tails = jnp.concatenate([returned[:, faces:], jnp.zeros((5, 128), f32)], axis=0)
    for place, pack in enumerate(packs):
        turned = [pltpu.roll(tails, (k - place) % 4 * edge, 1) for k in range(4)]
        above = jnp.where(
            group == 1, turned[1][1:2], jnp.where(group == 2, turned[2][0:1], jnp.where(group == 3, turned[3][2:3], 0.0))
        )
        below = jnp.where(
            group == 0, turned[0][0:1], jnp.where(group == 1, turned[1][2:3], jnp.where(group == 2, turned[2][1:2], 0.0))
        )
        above_sum = above_sum + pack[0:8] * jnp.broadcast_to(above, (memory, 128))
        below_sum = below_sum + pack[8:16] * jnp.broadcast_to(below, (memory, 128))
    both = above_sum + below_sum
    step_sum = lane_sum(far_step) + lane_sum(jnp.where(group < 2, both, 0.0))
    diff_sum = lane_sum(far_diff) + lane_sum(jnp.where(group < 2, 0.0, both))
    common = common_ref[...] + jnp.where(iota((8, 128), 0) == 6, placed_dots(step_sum, diff_sum), 0.0)
    for device in range(chunk_ref.shape[0]):
        chunk_ref[device] = common
    for code in range(1, 8):
        target = linear_device(code_bits(code))
        start = {1: 0, 2: face, 4: 2 * face}.get(code, faces)
        pieces = [returned[:, start : start + 128]]
        if code in (1, 2, 4):
            pieces.append(returned[:, start + 128 : start + 256])
        chunk_ref[target, 0 : 3 * len(pieces), :] = jnp.concatenate(pieces, axis=0)


def finish_kernel(sizes, atoms_total, recv_ref, order_ref, grad_ref, coords_ref, step_ref, diff_ref, new_ref, energy_ref):
    _, edge, _ = sizes
    faces, edges = slab_order(sizes)
    atoms = coords_ref.shape[1]
    memory = step_ref.shape[1]
    devices = recv_ref.shape[0]
    total = recv_ref[0]
    for device in range(1, devices):
        total = total + recv_ref[device]
    dots = jnp.broadcast_to(total[6:7, :], (memory, 128))
    gram = jnp.broadcast_to(total[7:8, :], (memory, 128))
    sub = iota((memory, 128), 0)
    lane = iota((memory, 128), 1)

    def pick(row, where):
        return jnp.broadcast_to(lane_sum(jnp.where(where, row, 0.0)), (memory, 128))

    def at(value, m):
        return jnp.broadcast_to(value[m : m + 1, :], (memory, 128))

    step_dots = pick(dots, lane == sub)
    diff_dots = pick(dots, lane == sub + memory)
    energy_ref[...] = lane_sum(jnp.where(iota((1, 128), 1) == 2 * memory, total[6:7, :], 0.0)) / atoms_total
    sy_col = [pick(gram, lane == sub * memory + j) for j in range(memory)]
    sy_row = [pick(gram, lane == j * memory + sub) for j in range(memory)]
    yy_col = [pick(gram, lane == memory * memory + sub * memory + j) for j in range(memory)]
    diagonal = pick(gram, lane == sub * (memory + 1))
    rho = 1.0 / diagonal
    last = memory - 1
    scaling = at(diagonal, last) / at(yy_col[last], last)
    left = step_dots
    alpha = jnp.zeros((memory, 128), f32)
    folded = diff_dots
    for m in reversed(range(memory)):
        value = at(left * rho, m)
        alpha = jnp.where(sub == m, value, alpha)
        left = left - value * sy_col[m]
        folded = folded - value * yy_col[m]
    left = diagonal * alpha - scaling * folded
    coef = jnp.zeros((memory, 128), f32)
    for m in range(memory):
        value = at(left * rho, m)
        coef = jnp.where(sub == m, value, coef)
        left = left - value * sy_row[m]
    diff_coef = -scaling * alpha

    blocks = {code: recv_ref[linear_device(tuple(-bit for bit in code_bits(code)))] for code in range(1, 8)}
    edge_lane = iota((8, 128), 1)
    tail = jnp.where(
        edge_lane < edge,
        blocks[3],
        jnp.where(edge_lane < 2 * edge, blocks[5], jnp.where(edge_lane < 3 * edge, blocks[6], blocks[7])),
    )
    tail = jnp.where(edge_lane < edges, tail, 0.0)
    pieces = []
    for code in (1, 2, 4):
        pieces += [blocks[code][0:3], blocks[code][3:6]]
    pieces.append(tail[0:3])
    returned = jnp.concatenate(pieces, axis=1)
    send = order_ref[:, : faces + 128]
    blocks = atoms // 128
    high = jnp.broadcast_to(send >> 7, (blocks, faces + 128)) == iota((blocks, faces + 128), 0)
    spread = [jnp.where(high, jnp.broadcast_to(returned[c : c + 1], high.shape), 0.0) for c in range(3)]
    back = jnp.concatenate(split_parts(jnp.concatenate(spread, axis=0), 2), axis=0)
    tiles = join_parts(dot_nt(back, row_one_hot(send & 127, 0, 128)), 3 * blocks, 2)
    added = [
        jnp.concatenate([tiles[c * blocks + block : c * blocks + block + 1] for block in range(blocks)], axis=1)
        for c in range(3)
    ]
    widen = atoms // 128
    for c in range(3):
        grad = grad_ref[c : c + 1, :] + added[c]
        mixed = jnp.tile(coef, (1, widen)) * step_ref[c] + jnp.tile(diff_coef, (1, widen)) * diff_ref[c]
        direction = jnp.tile(scaling[0:1], (1, widen)) * grad + jnp.sum(mixed, axis=0, keepdims=True)
        new_ref[c : c + 1, :] = coords_ref[c : c + 1, :] - step_length * direction


def call(kernel, outs, scratch, *args, limit_mib=16, space=pltpu.VMEM):
    if space == pltpu.HBM:
        args = [pltpu.with_memory_space_constraint(arg, pltpu.HBM) for arg in args]
    return pl.pallas_call(
        kernel,
        out_shape=[jax.ShapeDtypeStruct(shape, dtype) for shape, dtype in outs],
        in_specs=[pl.BlockSpec(memory_space=space)] * len(args),
        out_specs=[pl.BlockSpec(memory_space=pltpu.VMEM)] * len(outs),
        scratch_shapes=scratch,
        compiler_params=pltpu.CompilerParams(vmem_limit_bytes=limit_mib << 20),
    )(*args)


def on_device(
    coords,
    anchor,
    atom_types,
    halo_send,
    neighbours,
    live_counts,
    rep_coef,
    disp_coef,
    charge,
    step_history,
    grad_history,
):
    atoms = coords.shape[1]
    clusters = atoms // 8
    memory = step_history.shape[0]
    sizes = export_sizes(atoms)
    face, edge, corner = sizes
    faces, _ = slab_order(sizes)
    lanes = faces + 128
    wide = pl.cdiv(lanes, 1024) * 1024
    slots = neighbours.shape[1]
    devices = lax.axis_size("gx") * lax.axis_size("gy") * lax.axis_size("gz")
    assert edge == 32 and corner <= edge and face == 256 and memory == 8
    steps = step_history.transpose(1, 0, 2)
    diffs = grad_history.transpose(1, 0, 2)
    neigh = neighbours.T
    live = live_counts[None]
    rows = 6 * memory

    types, tables = atom_types[None], [table[None] for table in (rep_coef, disp_coef, charge)]
    pay_z, pay_y, pay_x, pay_e, order, coords_v, steps_v, diffs_v, anchor_v, neigh_v, live_v, *types_v = call(
        functools.partial(export_kernel, sizes),
        [((32, 128), f32)] * 2
        + [((16, 128), f32), ((32, 128), f32), ((1, wide), i32)]
        + [(value.shape, value.dtype) for value in (coords, steps, diffs, anchor, neigh, live, types, *tables)],
        [
            pltpu.VMEM((8, atoms), f32),
            pltpu.VMEM((1, wide), i32),
            pltpu.VMEM(halo_send.shape, i32),
            pltpu.SemaphoreType.DMA((11,)),
        ],
        halo_send, coords, types, *tables,
        steps, diffs, anchor, neigh, live,
        space=pltpu.HBM,
    )
    pe = shifted(pay_e, ("gy", "gz"), -1)
    py = shifted(pay_y, ("gy",), -1)
    pz = shifted(pay_z, ("gz",), -1)
    far_z, far_y, far_x = call(history_kernel, [((rows, face), f32)] * 3, [], steps_v, diffs_v, order)
    fx = shifted(far_x, ("gx",), -1)
    fy = shifted(far_y, ("gy",), -1)
    fz = shifted(far_z, ("gz",), -1)
    tiles, other = call(
        local_kernel,
        [((48, clusters), f32), ((48, slots * clusters), f32)],
        [],
        coords_v, *types_v, neigh_v,
    )
    pay_x, far_e = call(
        functools.partial(merge_kernel, edge),
        [((24, 128), f32), ((48, 128), f32)],
        [],
        pay_x, pz, py, pe,
        limit_mib=4,
    )
    px = shifted(pay_x, ("gx",), -1)
    fe = shifted(far_e, ("gx",), -1)
    near, halo_select, low_select = call(
        functools.partial(prep_kernel, sizes),
        [((48, slots * clusters), f32)] + [((128, slots * clusters), bf16)] * 2,
        [],
        other, neigh_v, pz, py, pe,
    )
    (gram,) = call(gram_kernel, [((memory, 128), f32)], [], steps_v, diffs_v, limit_mib=8)
    grad, returned, common = call(
        functools.partial(pair_kernel, sizes),
        [((3, atoms), f32), ((3, lanes), f32), ((8, 128), f32)],
        [pltpu.VMEM((48, slots * clusters), f32), pltpu.VMEM((24, slots * clusters), f32)],
        tiles, near, low_select, halo_select, gram, px, neigh_v, live_v, coords_v, anchor_v, steps_v, diffs_v,
        limit_mib=16,
    )
    (chunks,) = call(
        functools.partial(chunk_kernel, sizes),
        [((devices, 8, 128), f32)],
        [],
        common, returned, fz, fy, fx, fe, pe,
        limit_mib=24,
    )
    received = lax.all_to_all(chunks, AXES, 0, 0, tiled=True)
    new_coords, energy = call(
        functools.partial(finish_kernel, sizes, atoms * devices),
        [((3, atoms), f32), ((1, 1), f32)],
        [],
        received, order, grad, coords_v, steps_v, diffs_v,
    )
    return (new_coords, energy[0, 0])


def solution(mesh):
    placed = (
        P(None, AXES),
        P(None, AXES),
        P(AXES),
        P(AXES),
        P(AXES, None),
        P(AXES),
        P(),
        P(),
        P(),
        P(None, None, AXES),
        P(None, None, AXES),
    )

    return jax.shard_map(
        on_device,
        mesh=mesh,
        in_specs=placed,
        out_specs=(P(None, AXES), P()),
        check_vma=False,
    )
```
